256 devices in a mesh: blk: 16 (over x, y_hi, core), grp: 16 (over y_lo, z).
Axes of the slice: x: 4, y: 4 (y_hi: 2, y_lo: 2; y = y_hi * 2 + y_lo), z: 8, core: 2. Of those that a mesh axis runs over, the one named last changes fastest.
Arguments:
- amplitudes: bfloat16 [896, 4, 896], P('blk', None, 'grp'), may hold values from -6 to 6
- grid_factor: bfloat16 [8192, 896], P(('blk', 'grp')), may hold values from -0.1875 to 0.1875
- metric: float32 [8192, 16, 512], P('blk', 'grp'), may hold values from -0.625 to 0.625
- virt_energy: float32 [896], replicated, may hold values from 0.2 to 4
- pair_energy: float32 [4], replicated, may hold values from -2 to -0.5
Outputs:
- residual: float32 [896, 4, 896], P('blk', None, 'grp')
The draws below stay inside these ranges and needn't reach their ends.
All inputs are finite; a program needn't handle non-finite values.
Results may differ from the reference program's by a relative error of at most 0.005.
Values may be sent and summed in bfloat16 or wider, within the bound.
A program may use at most 64 MiB of HBM per device.

```python
import math
import jax
import jax.numpy as jnp
from jax import lax

NV = 896
PTS = 32
OP = 4
NG = 8192
N_BLK = 16
N_GRP = 16


def block_levels(stream_key, extent, pieces, least, top_value):
    gain = 1.0
    for position, blocks in pieces:
        heights = jax.random.uniform(jax.random.fold_in(jax.random.fold_in(stream_key, 6), position), (blocks,), jnp.float32, least / len(pieces), top_value / len(pieces))
        gain = gain * jnp.repeat(jnp.exp(heights), extent[position] // blocks).reshape((-1,) + (1,) * (len(extent) - 1 - position))
    return gain


def normal_values(stream_key, extent, width, most, cuts=(), kind=jnp.bfloat16):
    result = jax.random.normal(stream_key, extent, jnp.float32) * width
    if len(cuts) > 0:
        result = block_levels(stream_key, extent, cuts, -0.22, 0.18) * result
    return jnp.clip(result, min=-most, max=most).astype(kind)


def setup_inputs(seed: int = 0) -> dict:
    key_list = jax.random.split(jax.random.key(seed), 6)
    return {
        "amplitudes": normal_values(key_list[0], (NV, OP, NV), 1.0, 6.0, ((0, 16), (2, 16))),
        "grid_factor": normal_values(key_list[1], (NG, NV), NV ** -0.5, 0.1875, ((0, 256),)),
        "metric": normal_values(key_list[2], (NG, N_GRP, N_BLK * PTS), ((NG // NV) ** 2) ** -0.5, 0.625, ((0, 16), (1, 16)), jnp.float32),
        "virt_energy": jnp.clip(jnp.exp(jax.random.uniform(key_list[3], (NV,), jnp.float32, math.log(0.2), math.log(4.0))), 0.2, 4.0),
        "pair_energy": jnp.clip(jax.random.uniform(key_list[4], (OP,), jnp.float32, -2.0, -0.5), -2.0, -0.5),
    }


def reference(amplitudes, grid_factor, metric, virt_energy, pair_energy):
    metric_full = jnp.transpose(metric.reshape(NG, N_GRP, N_BLK, PTS), (0, 2, 1, 3)).reshape(NG, NG)
    factor_split = grid_factor.reshape(N_BLK, N_GRP, PTS, NV)

    def one_pair(pair_amp):
        left = jnp.dot(grid_factor, pair_amp, preferred_element_type=jnp.float32).astype(jnp.bfloat16)
        products = jnp.dot(left, grid_factor.T, preferred_element_type=jnp.float32)
        weighted = (metric_full * products).astype(jnp.bfloat16).reshape(NG, N_BLK, N_GRP, PTS)

        def add_group(summed, group):
            block = lax.dynamic_index_in_dim(weighted, group, 2, keepdims=False).astype(jnp.float32)
            rows = lax.dynamic_index_in_dim(factor_split, group, 1, keepdims=False).astype(jnp.float32)
            partial_sum = jnp.einsum("pbr,brv->pv", block, rows, precision=lax.Precision.HIGHEST)
            rounded = lax.optimization_barrier(partial_sum.astype(jnp.bfloat16))
            return summed + rounded.astype(jnp.float32), None

        summed, unused = lax.scan(add_group, jnp.zeros((NG, NV), jnp.float32), jnp.arange(N_GRP, dtype=jnp.int32))
        mixed = summed.astype(jnp.bfloat16)
        return jnp.dot(grid_factor.T, mixed, preferred_element_type=jnp.float32)

    ladder = lax.map(one_pair, jnp.transpose(amplitudes, (1, 0, 2)))
    ladder = jnp.transpose(ladder, (1, 0, 2))
    denominator = virt_energy[:, None, None] + virt_energy[None, None, :] - pair_energy[None, :, None]
    return denominator * amplitudes.astype(jnp.float32) + ladder
```

```python
import functools

import jax
import jax.numpy as jnp
from jax import lax
from jax.experimental import pallas as pl
from jax.experimental.pallas import tpu as pltpu
from jax.sharding import PartitionSpec as P

MESH = pl.DeviceIdType.MESH
F32 = jnp.float32
BF16 = jnp.bfloat16
SEMS = 160


class Links:
    def __init__(self, send, recv):
        self.send, self.recv, self.ids, self.open = send, recv, {}, []

    def index(self, key):
        return self.ids.setdefault(key, len(self.ids))

    def copy(self, key, src, dst, dev):
        i = self.index(key)
        return pltpu.make_async_remote_copy(
            src_ref=src, dst_ref=dst, send_sem=self.send.at[i], recv_sem=self.recv.at[i],
            device_id=dev, device_id_type=MESH,
        )

    def start(self, key, src, dst, dev):
        c = self.copy(key, src, dst, dev)
        c.start()
        self.open.append(c)

    def arrived(self, key, dst, dev):
        self.copy(key, dst, dst, dev).wait_recv()

    def close(self):
        for c in self.open:
            c.wait_send()


def kernel(
    tt_ref, x_ref, z_hbm, out_ref,
    tsw, town, tall, xq, xqt, xp, xpt, zb, right, w, mp,
    e1s, e1r, e2s, e2r, eys, eyr, lad, fs, fr, fins, finr,
    send, recv, zsem,
):
    b, g = lax.axis_index("blk"), lax.axis_index("grp")
    core, yh, x = b % 2, (b // 2) % 2, b // 4
    yl, z = g // 8, g % 8
    m = x * 2 + yh
    net = Links(send, recv)

    mate = {"blk": b + 1 - 2 * core, "grp": g}
    xn = {"blk": ((x + 1) % 4) * 4 + b % 4, "grp": g}
    xv = {"blk": ((x + 3) % 4) * 4 + b % 4, "grp": g}
    yp = {"blk": b + 2 - 4 * yh, "grp": g}
    zn = {"blk": b, "grp": yl * 8 + (z + 1) % 8}
    zv = {"blk": b, "grp": yl * 8 + (z + 7) % 8}
    yn = {"blk": b, "grp": (1 - yl) * 8 + z}

    def peer(r):
        return {"blk": b, "grp": (g + r) % 16}

    zcopy = pltpu.make_async_copy(z_hbm.at[:, 0, :], zb.at[core], zsem)
    zcopy.start()

    barrier = pltpu.get_barrier_semaphore()
    near = [mate, xn, xv, yp] + [peer(r) for r in range(1, 16)]
    for dev in near:
        pl.semaphore_signal(barrier, inc=1, device_id=dev, device_id_type=MESH)
    pl.semaphore_wait(barrier, len(near))

    net.start("tsw", tt_ref.at[pl.ds(2 * (1 - core), 2)], tsw, mate)
    net.start("xqy", x_ref, xq.at[m, core], yp)
    net.start("xqn0", x_ref, xq.at[m, core], xn)
    net.start("xqv0", x_ref, xq.at[m, core], xv)
    xq[m, core] = x_ref[...]
    xp[core, g] = x_ref[...]

    net.arrived("tsw", tsw, mate)
    for k in range(2):
        mine = (tt_ref[2 * core + k].astype(F32) + tsw[k].astype(F32)).astype(BF16)
        town[k] = mine
        tall[k, g] = mine
    for k in range(2):
        for r in range(1, 16):
            net.start(("t", k, r), town.at[k], tall.at[k, g], peer(r))

    net.start("zsw", z_hbm.at[:, 0, :], zb.at[core], mate)
    net.start("xpy", x_ref, xp.at[core, g], yn)
    net.start(("xpn", 0, 1), x_ref, xp.at[core, g], zn)
    net.start(("xpv", 0, 1), x_ref, xp.at[core, g], zv)

    my = x * 2 + 1 - yh
    net.arrived("xqy", xq.at[my, core], yp)
    net.start("xqn1", xq.at[my, core], xq.at[my, core], xn)
    net.start("xqv1", xq.at[my, core], xq.at[my, core], xv)
    xm1, xp1, xp2 = (x + 3) % 4, (x + 1) % 4, (x + 2) % 4

    def at_y(o):
        return 1 - yh if o == 1 else yh

    def xqs(xx, o):
        return xq.at[xx * 2 + at_y(o), core]

    net.arrived("xqn0", xqs(xm1, 0), xv)
    net.start("xqf0", xqs(xm1, 0), xqs(xm1, 0), xn)
    net.arrived("xqv0", xqs(xp1, 0), xn)
    net.arrived("xqv1", xqs(xp1, 1), xn)
    net.start("xqf1", xqs(xp1, 1), xqs(xp1, 1), xv)
    net.arrived("xqn1", xqs(xm1, 1), xv)
    net.arrived("xqf0", xqs(xp2, 0), xv)
    net.arrived("xqf1", xqs(xp2, 1), xn)
    net.start("xqm", xq.at[:, core], xq.at[:, core], mate)

    def rows(xx, o):
        return pl.ds(pl.multiple_of((xx * 2 + at_y(o)) * 112, 16), 112)

    def xpa(dyl, dz):
        g_from = ((1 - yl) if dyl else yl) * 8 + (z + dz + 8) % 8
        return xp.at[core, g_from]

    net.arrived("xqm", xq.at[:, 1 - core], mate)
    for k in range(2):
        for r in range(1, 16):
            net.arrived(("t", k, r), tall.at[k, (g - r + 16) % 16], peer(16 - r))
        t = jnp.concatenate([tall[k, j].astype(F32)[:56] for j in range(16)], axis=0)
        rt = lax.dot_general(
            t.astype(BF16), xq[...].reshape(512, 896), (((0,), (1,)), ((), ())),
            preferred_element_type=F32,
        )
        right[k, rows(x, 0)] = jnp.concatenate([rt[:56], rt[64:120]], axis=0).astype(BF16)
        own = right.at[k, rows(x, 0)]
        net.start(("ry", k), own, own, yp)
        net.start(("rn", k, 0), own, own, xn)
        net.start(("rv", k, 0), own, own, xv)
        if k == 0:
            net.arrived("xpy", xpa(1, 0), yn)
            net.start(("xpn", 1, 1), xpa(1, 0), xpa(1, 0), zn)
            net.start(("xpv", 1, 1), xpa(1, 0), xpa(1, 0), zv)

    def xp_step(s):
        for dyl in range(2):
            net.arrived(("xpn", dyl, s), xpa(dyl, -s), zv)
            if s < 4:
                net.start(("xpn", dyl, s + 1), xpa(dyl, -s), xpa(dyl, -s), zn)
            if s < 4:
                net.arrived(("xpv", dyl, s), xpa(dyl, s), zn)
                if s < 3:
                    net.start(("xpv", dyl, s + 1), xpa(dyl, s), xpa(dyl, s), zv)

    def r_y(k):
        part = right.at[k, rows(x, 1)]
        net.arrived(("ry", k), part, yp)
        net.start(("rn", k, 1), part, part, xn)
        net.start(("rv", k, 1), part, part, xv)

    def r_forward(k, o):
        net.arrived(("rn", k, o), right.at[k, rows(xm1, o)], xv)
        part = right.at[k, rows(xm1, o), pl.ds(0, 256)]
        net.start(("rfn", k, o), part, part, xn)
        net.arrived(("rv", k, o), right.at[k, rows(xp1, o)], xn)
        part = right.at[k, rows(xp1, o), pl.ds(256, 256)]
        net.start(("rfv", k, o), part, part, xv)

    def r_last(k):
        for o in range(2):
            net.arrived(("rfn", k, o), right.at[k, rows(xp2, o), pl.ds(0, 256)], xv)
            net.arrived(("rfv", k, o), right.at[k, rows(xp2, o), pl.ds(256, 256)], xn)

    def compute(k):
        def tile(t, carry):
            c, h = t // 2, t % 2
            p = jnp.dot(
                xp[c, pl.ds(8 * h, 8)].reshape(256, 896), right[k], preferred_element_type=F32
            )
            zt = zb[c, pl.ds(pl.multiple_of(256 * h, 256), 256), :]
            w[pl.ds(pl.multiple_of(256 * t, 256), 256), :] = (zt * p).astype(BF16)
            return carry

        lax.fori_loop(0, 4, tile, 0)

        def mix(t, carry):
            a = pl.ds(pl.multiple_of(128 * t, 128), 128)
            mp[k, a, :] = jnp.dot(xpt[a, :], w[...], preferred_element_type=F32)
            return carry

        lax.fori_loop(0, 7, mix, 0)

    def e_one(k):
        for o in (1, 0):
            v = mp[k, rows(xp2, o), :]
            e1s[k, o, 0] = v[:, :256].astype(BF16)
            e1s[k, o, 1] = v[:, 256:].astype(BF16)
            net.start(("e1n", k, o), e1s.at[k, o, 0], e1r.at[k, o, 0], xn)
            net.start(("e1v", k, o), e1s.at[k, o, 1], e1r.at[k, o, 1], xv)

    def e_two(k):
        for o in (1, 0):
            net.arrived(("e1n", k, o), e1r.at[k, o, 0], xv)
            v = mp[k, rows(xp1, o), :]
            e2s[k, o, 0] = jnp.concatenate(
                [v[:, :256] + e1r[k, o, 0].astype(F32), v[:, 256:]], axis=1
            ).astype(BF16)
            net.start(("e2n", k, o), e2s.at[k, o, 0], e2r.at[k, o, 0], xn)
            net.arrived(("e1v", k, o), e1r.at[k, o, 1], xn)
            v = mp[k, rows(xm1, o), :]
            e2s[k, o, 1] = jnp.concatenate(
                [v[:, :256], v[:, 256:] + e1r[k, o, 1].astype(F32)], axis=1
            ).astype(BF16)
            net.start(("e2v", k, o), e2s.at[k, o, 1], e2r.at[k, o, 1], xv)

    def e_three(k):
        for o in (1, 0):
            net.arrived(("e2n", k, o), e2r.at[k, o, 0], xv)
            net.arrived(("e2v", k, o), e2r.at[k, o, 1], xn)
            v = mp[k, rows(x, o), :] + e2r[k, o, 0].astype(F32) + e2r[k, o, 1].astype(F32)
            if o == 1:
                eys[k] = v.astype(BF16)
                net.start(("ey", k), eys.at[k], eyr.at[k], yp)
            else:
                mp[k, rows(x, 0), :] = v

    def ladder(k):
        net.arrived(("ey", k), eyr.at[k], yp)
        v = mp[k, rows(x, 0), :] + eyr[k].astype(F32)
        gap = jnp.zeros((8, 512), F32)
        v = jnp.concatenate([v[:56], gap, v[56:], gap], axis=0).astype(BF16)
        lad[...] = lax.dot_general(
            xqt[...], v, (((1,), (1,)), ((), ())), preferred_element_type=F32
        )
        gap = jnp.zeros((8, 128), F32)
        for j in range(16):
            fs[k, j] = jnp.concatenate([lad[56 * j : 56 * j + 56, :], gap], axis=0).astype(BF16)
        for r in range(1, 16):
            net.start(("f", k, r), fs.at[k, (g + r) % 16], fr.at[k, r], peer(r))
        fins[k, pl.ds(0, 56), :] = lad[pl.ds(pl.multiple_of(g * 56, 8), 56), :]
        fins[k, pl.ds(56, 8), :] = gap

    xp_step(1)
    r_y(0)
    r_forward(0, 0)
    xp_step(2)
    r_y(1)
    r_forward(0, 1)
    xqt[...] = jnp.transpose(xq[...].reshape(512, 896))
    xp_step(3)
    r_forward(1, 0)
    xp_step(4)
    net.start("xpm", xp.at[core], xp.at[core], mate)
    r_forward(1, 1)
    zcopy.wait()
    net.arrived("zsw", zb.at[1 - core], mate)
    net.arrived("xpm", xp.at[1 - core], mate)
    for t in range(4):
        xpt[:, 256 * t : 256 * t + 256] = jnp.transpose(
            xp[t // 2, pl.ds(8 * (t % 2), 8)].reshape(256, 896)
        )
    r_last(0)
    compute(0)
    e_one(0)
    r_last(1)
    compute(1)
    e_one(1)
    e_two(0)
    e_two(1)
    e_three(0)
    e_three(1)
    ladder(0)
    ladder(1)
    for k in range(2):
        total = fins[k]
        for r in range(1, 16):
            net.arrived(("f", k, r), fr.at[k, r], peer(16 - r))
            total = total + fr[k, r].astype(F32)
        fins[k] = total
        net.start(("fin", k), fins.at[k], finr.at[k], mate)
    for k in range(2):
        out_ref[2 * core + k] = fins[k]
    for k in range(2):
        net.arrived(("fin", k), finr.at[k], mate)
        out_ref[2 * (1 - core) + k] = finr[k]
    net.close()


def local(amplitudes, grid_factor, metric, virt_energy, pair_energy):
    core = lax.axis_index("blk") % 2
    t = jnp.pad(jnp.transpose(amplitudes, (1, 2, 0)), ((0, 0), (0, 8), (0, 8)))
    tt = jnp.concatenate(
        [jnp.where(core == 0, t, jnp.zeros_like(t)), jnp.where(core == 1, t, jnp.zeros_like(t))],
        axis=2,
    )
    vm = pl.BlockSpec(memory_space=pltpu.VMEM)
    out = pl.pallas_call(
        kernel,
        out_shape=jax.ShapeDtypeStruct((4, 64, 128), F32),
        in_specs=[vm, vm, pl.BlockSpec(memory_space=pl.ANY)],
        out_specs=vm,
        scratch_shapes=[
            pltpu.VMEM((2, 64, 128), BF16),
            pltpu.VMEM((2, 64, 128), BF16),
            pltpu.VMEM((2, 16, 64, 128), BF16),
            pltpu.VMEM((8, 2, 32, 896), BF16),
            pltpu.VMEM((896, 512), BF16),
            pltpu.VMEM((2, 16, 32, 896), BF16),
            pltpu.VMEM((896, 1024), BF16),
            pltpu.VMEM((2, 512, 512), F32),
            pltpu.VMEM((2, 896, 512), BF16),
            pltpu.VMEM((1024, 512), BF16),
            pltpu.VMEM((2, 896, 512), F32),
            pltpu.VMEM((2, 2, 2, 112, 256), BF16),
            pltpu.VMEM((2, 2, 2, 112, 256), BF16),
            pltpu.VMEM((2, 2, 2, 112, 512), BF16),
            pltpu.VMEM((2, 2, 2, 112, 512), BF16),
            pltpu.VMEM((2, 112, 512), BF16),
            pltpu.VMEM((2, 112, 512), BF16),
            pltpu.VMEM((896, 128), F32),
            pltpu.VMEM((2, 16, 64, 128), BF16),
            pltpu.VMEM((2, 16, 64, 128), BF16),
            pltpu.VMEM((2, 64, 128), F32),
            pltpu.VMEM((2, 64, 128), F32),
            pltpu.SemaphoreType.DMA((SEMS,)),
            pltpu.SemaphoreType.DMA((SEMS,)),
            pltpu.SemaphoreType.DMA,
        ],
        compiler_params=pltpu.CompilerParams(
            collective_id=0, has_side_effects=True, vmem_limit_bytes=48 * 1024 * 1024
        ),
    )(tt, grid_factor, metric)
    ladder = jnp.where(core == 0, out[:, :56, :56], out[:, :56, 64:120])
    ladder = jnp.transpose(ladder, (2, 0, 1))
    rows, cols = amplitudes.shape[0], amplitudes.shape[2]
    first = lax.dynamic_slice_in_dim(virt_energy, lax.axis_index("blk") * rows, rows)
    second = lax.dynamic_slice_in_dim(virt_energy, lax.axis_index("grp") * cols, cols)
    denominator = first[:, None, None] + second[None, None, :] - pair_energy[None, :, None]
    return denominator * amplitudes.astype(F32) + ladder


def solution(mesh):
    in_specs = (P("blk", None, "grp"), P(("blk", "grp"), None), P("blk", "grp", None), P(), P())
    return jax.shard_map(
        local, mesh=mesh, in_specs=in_specs, out_specs=P("blk", None, "grp"), check_vma=False
    )
```

```python
import functools

import jax
import jax.numpy as jnp
from jax import lax
from jax.experimental import pallas as pl
from jax.experimental.pallas import tpu as pltpu
from jax.sharding import PartitionSpec as P

MESH = pl.DeviceIdType.MESH
F32 = jnp.float32
BF16 = jnp.bfloat16
SEMS = 200


class Links:
    def __init__(self, send, recv):
        self.send, self.recv, self.ids, self.open = send, recv, {}, []

    def index(self, key):
        assert len(self.ids) < SEMS
        return self.ids.setdefault(key, len(self.ids))

    def copy(self, key, src, dst, dev):
        i = self.index(key)
        return pltpu.make_async_remote_copy(
            src_ref=src, dst_ref=dst, send_sem=self.send.at[i], recv_sem=self.recv.at[i],
            device_id=dev, device_id_type=MESH,
        )

    def start(self, key, src, dst, dev):
        c = self.copy(key, src, dst, dev)
        c.start()
        self.open.append(c)

    def arrived(self, key, dst, dev):
        self.copy(key, dst, dst, dev).wait_recv()

    def close(self):
        for c in self.open:
            c.wait_send()


def kernel(
    tt_ref, x_ref, z_hbm, out_ref,
    tall, xq, xqt, xp, xpt, zb, right, w, mp,
    e1s, e1r, e2s, e2r, e3s, e3r, eys, eyr, lad, fs, fy, fr, fins, finr,
    send, recv, zsem,
):
    b, g = lax.axis_index("blk"), lax.axis_index("grp")
    core, yh, x = b % 2, (b // 2) % 2, b // 4
    yl, z = g // 8, g % 8
    m = x * 2 + yh
    net = Links(send, recv)

    def at(dx, dy, dc=0):
        yy = 1 - yh if dy else yh
        cc = 1 - core if dc else core
        return {"blk": ((x + dx + 4) % 4) * 4 + yy * 2 + cc, "grp": g}

    def up(dz, dyl=0, dc=0):
        return {
            "blk": b + 1 - 2 * core if dc else b,
            "grp": ((1 - yl) if dyl else yl) * 8 + (z + dz) % 8,
        }

    mate, yp = at(0, 0, 1), at(0, 1)
    zn, zv, yn = up(1), up(7), up(0, 1)
    around = [(2, 1), (3, 1), (1, 1), (2, 0), (3, 0), (1, 0)]

    def rows(dx, o, first=0, count=112):
        yy = 1 - yh if o else yh
        return pl.ds(pl.multiple_of((((x + dx + 4) % 4) * 2 + yy) * 112 + first, 16), count)

    def xqa(dx, dy):
        return xq.at[((x + dx + 4) % 4) * 2 + ((1 - yh) if dy else yh), core]

    def gi(dz, dyl):
        return ((1 - yl) if dyl else yl) * 8 + (z + dz + 8) % 8

    def xpa(dyl, dz):
        return xp.at[core, gi(dz, dyl)]

    zcopy = pltpu.make_async_copy(z_hbm.at[:, 0, :], zb.at[core], zsem)
    zcopy.start()

    barrier = pltpu.get_barrier_semaphore()
    near = [mate, yn] + [at(dx, 0) for dx in range(1, 4)]
    near += [yp] + [up(dz, 0, dc) for dz in range(1, 8) for dc in range(2)]
    with jax.named_scope("barrier"):
        for dev in near:
            pl.semaphore_signal(barrier, inc=1, device_id=dev, device_id_type=MESH)
        pl.semaphore_wait(barrier, len(near))

    far = (4, 3, 5, 2, 6, 1, 7)

    def t_send(k):
        net.start(("t", k, 0, 1), tt_ref.at[2 * (1 - core) + k], tall.at[k, core, g], mate)
        for dz in far:
            for dc in range(2):
                pair = 2 * ((1 - core) if dc else core) + k
                net.start(("t", k, dz, dc), tt_ref.at[pair], tall.at[k, core, g], up(dz, 0, dc))
        tall[k, core, g] = tt_ref[2 * core + k]

    def t_forward(k, dz):
        j = gi(-dz, 0)
        for dc in range(2):
            if dz or dc:
                part = tall.at[k, (1 - core) if dc else core, j]
                net.arrived(("t", k, dz, dc), part, up(8 - dz, 0, dc))
        net.start(("ty", k, dz), tall.at[k, :, j], tall.at[k, :, j], yn)

    t_send(0)
    net.start("xpy", x_ref, xpa(0, 0), yn)
    for dx, dy in ((0, 1), (1, 0), (3, 0), (2, 0)):
        net.start(("xq", dx, dy), x_ref, xqa(0, 0), at(dx, dy))
    net.start(("xqm", 0, 0), x_ref, xqa(0, 0), mate)
    net.start(("xpn", 0, 1), x_ref, xpa(0, 0), zn)
    net.start(("xpv", 0, 1), x_ref, xpa(0, 0), zv)
    net.start(("xpm", 0, 0), x_ref, xpa(0, 0), mate)
    xq[m, core] = x_ref[...]
    xp[core, g] = x_ref[...]

    def xq_forward(dx, dy):
        part = xqa(-dx, dy)
        net.arrived(("xq", dx, dy), part, at(4 - dx, 0 if dx else dy))
        if (dx, dy) == (0, 1):
            for to in (1, 3, 2):
                net.start(("xq", to, 1), part, part, at(to, 0))
        net.start(("xqm", dx, dy), part, part, mate)

    lane = lax.broadcasted_iota(jnp.int32, (512, 128), 1)

    def first(k):
        for dz in (0,) + far:
            net.arrived(("ty", k, dz), tall.at[k, :, gi(-dz, 1)], yn)
        one = tall[k, 0].reshape(512, 128).astype(F32)
        two = tall[k, 1].reshape(512, 128).astype(F32)
        top = jnp.where(lane < 64, one, pltpu.roll(two, 64, 1))
        low = jnp.where(lane < 64, pltpu.roll(one, 64, 1), two)
        t = jnp.concatenate(
            [v for j in range(16) for v in (top[32 * j : 32 * j + 32], low[32 * j : 32 * j + 24])],
            axis=0,
        )
        rt = lax.dot_general(
            t.astype(BF16), xq[...].reshape(512, 896), (((0,), (1,)), ((), ())),
            preferred_element_type=F32,
        )
        right[k, rows(0, 0)] = jnp.concatenate([rt[:56], rt[64:120]], axis=0).astype(BF16)
        own = right.at[k, rows(0, 0)]
        net.start(("ry", k, 0), own, own, yp)
        for dx in (1, 3, 2):
            net.start(("rx", k, dx), own, own, at(dx, 0))

    def xp_mate(dyl, dz):
        net.start(("xpm", dyl, dz), xpa(dyl, dz), xpa(dyl, dz), mate)

    def xp_y():
        part = xpa(1, 0)
        net.arrived("xpy", part, yn)
        net.start(("xpn", 1, 1), part, part, zn)
        net.start(("xpv", 1, 1), part, part, zv)
        xp_mate(1, 0)

    def xp_step(s, dyl):
        if s < 4 or dyl == 0:
            part = xpa(dyl, -s)
            net.arrived(("xpn", dyl, s), part, zv)
            if s < 3 or (s == 3 and dyl == 0):
                net.start(("xpn", dyl, s + 1), part, part, zn)
            xp_mate(dyl, -s)
        if s < 4 or dyl == 1:
            part = xpa(dyl, s)
            net.arrived(("xpv", dyl, s), part, zn)
            if s < 3 or (s == 3 and dyl == 1):
                net.start(("xpv", dyl, s + 1), part, part, zv)
            xp_mate(dyl, s)

    def r_y(k):
        net.arrived(("ry", k, 0), right.at[k, rows(0, 1)], yp)
        part = right.at[k, rows(0, 1, 0, 48)]
        for dx in (1, 3, 2):
            net.start(("rz", k, dx), part, part, at(dx, 0))

    def r_x(k, *ways):
        for dx in ways:
            net.arrived(("rx", k, dx), right.at[k, rows(-dx, 0)], at(4 - dx, 0))
            part = right.at[k, rows(-dx, 0, 48, 64)]
            net.start(("ry", k, dx), part, part, yp)

    def r_last(k):
        for dx in (1, 3, 2):
            net.arrived(("rz", k, dx), right.at[k, rows(-dx, 1, 0, 48)], at(4 - dx, 0))
        for dx in (1, 3, 2):
            net.arrived(("ry", k, dx), right.at[k, rows(-dx, 1, 48, 64)], yp)

    def weigh(k, c):
        p = jnp.dot(xp[c].reshape(512, 896), right[k], preferred_element_type=F32)
        w[512 * c : 512 * c + 512, :] = (zb[c] * p).astype(BF16)

    def mix(k, t):
        a = pl.ds(448 * t, 448)
        mp[k, a, :] = jnp.dot(xpt[a, :], w[...], preferred_element_type=F32)

    order = (2, 1, 3, 0)

    def e_start(k):
        for i, dx in enumerate(order):
            eys[k, i] = mp[k, rows(dx, 1, 48, 64), :].astype(BF16)
            net.start(("ey", k, dx), eys.at[k, i], eyr.at[k, i], yp)
            if dx:
                for o in range(2):
                    e1s[k, i, o] = mp[k, rows(dx, o, 0, 48), :].astype(BF16)
                net.start(("e1", k, dx), e1s.at[k, i], e1r.at[k, i], at(dx, 0))

    def e_y(k, dx):
        i = order.index(dx)
        net.arrived(("ey", k, dx), eyr.at[k, i], yp)
        return mp[k, rows(dx, 0, 48, 64), :] + eyr[k, i].astype(F32)

    def e_two(k):
        for i, dx in enumerate(order[:3]):
            e2s[k, i] = e_y(k, dx).astype(BF16)
            net.start(("e2", k, dx), e2s.at[k, i], e2r.at[k, i], at(dx, 0))

    def e_three(k):
        v = mp[k, rows(0, 1, 0, 48), :]
        for i, dx in enumerate(order[:3]):
            net.arrived(("e1", k, dx), e1r.at[k, i], at(4 - dx, 0))
            v = v + e1r[k, i, 1].astype(F32)
        e3s[k] = v.astype(BF16)
        net.start(("e3", k), e3s.at[k], e3r.at[k], yp)

    def e_last(k):
        v = e_y(k, 0)
        for i, dx in enumerate(order[:3]):
            net.arrived(("e2", k, dx), e2r.at[k, i], at(4 - dx, 0))
            v = v + e2r[k, i].astype(F32)
        u = mp[k, rows(0, 0, 0, 48), :]
        for i in range(3):
            u = u + e1r[k, i, 0].astype(F32)
        net.arrived(("e3", k), e3r.at[k], yp)
        return jnp.concatenate([u + e3r[k].astype(F32), v], axis=0)

    def ladder(k, v):
        gap = jnp.zeros((8, 512), F32)
        v = jnp.concatenate([v[:56], gap, v[56:], gap], axis=0).astype(BF16)
        lad[k] = lax.dot_general(
            xqt[...], v, (((1,), (1,)), ((), ())), preferred_element_type=F32
        )
        gap = jnp.zeros((8, 128), F32)
        for dz in range(8):
            j = gi(dz, 1)
            v = lad[k, pl.ds(pl.multiple_of(j * 56, 8), 56), :]
            fs[k, j] = jnp.concatenate([v, gap], axis=0).astype(BF16)
        for dz in far + (0,):
            net.start(("fy", k, dz), fs.at[k, gi(dz, 1)], fy.at[k, dz], yn)

    def fold(k):
        for dz in far + (0,):
            j = gi(dz, 0)
            net.arrived(("fy", k, dz), fy.at[k, dz], yn)
            v = lad[k, pl.ds(pl.multiple_of(j * 56, 8), 56), :] + fy[k, dz, 0:56].astype(F32)
            v = jnp.concatenate([v, jnp.zeros((8, 128), F32)], axis=0)
            if dz:
                fs[k, j] = v.astype(BF16)
                net.start(("f", k, dz), fs.at[k, j], fr.at[k, dz], up(dz))
            else:
                fins[k] = v

    def scoped(name, f, *args):
        with jax.named_scope(name):
            return f(*args)

    scoped("xp_y", xp_y)
    scoped("xq_y", xq_forward, 0, 1)
    with jax.named_scope("t0_xq"):
        t_forward(0, 0)
        for i, dz in enumerate(far[::-1]):
            t_forward(0, dz)
            if i < 3:
                xq_forward(*around[::-1][i])
    scoped("xp_step10", xp_step, 1, 0)
    scoped("xp_step11", xp_step, 1, 1)
    t_send(1)
    with jax.named_scope("xq_far"):
        for dx, dy in around[2::-1]:
            xq_forward(dx, dy)
    with jax.named_scope("xqm_wait"):
        for dx, dy in around + [(0, 1), (0, 0)]:
            part = xq.at[((x - dx + 4) % 4) * 2 + ((1 - yh) if dy else yh), 1 - core]
            net.arrived(("xqm", dx, dy), part, mate)
    scoped("first0", first, 0)
    scoped("xp_step20", xp_step, 2, 0)
    scoped("xp_step21", xp_step, 2, 1)
    with jax.named_scope("xqt"):
        xqt[...] = jnp.transpose(xq[...].reshape(512, 896))
    net.start("zsw", z_hbm.at[:, 0, :], zb.at[core], mate)
    with jax.named_scope("t1"):
        for dz in (0,) + far[::-1]:
            t_forward(1, dz)
    scoped("r_x01", r_x, 0, 1)
    scoped("xp_step30", xp_step, 3, 0)
    scoped("r_x03", r_x, 0, 3)
    scoped("xp_step31", xp_step, 3, 1)
    scoped("r_y0", r_y, 0)
    scoped("r_x02", r_x, 0, 2)
    scoped("first1", first, 1)
    scoped("xp_step40", xp_step, 4, 0)
    scoped("xp_step41", xp_step, 4, 1)
    with jax.named_scope("z_wait"):
        zcopy.wait()
        net.arrived("zsw", zb.at[1 - core], mate)
    scoped("r_x11", r_x, 1, 1)
    with jax.named_scope("xpm_wait"):
        for s in range(-4, 5):
            for dyl in range(2):
                if (s, dyl) not in ((4, 0), (-4, 1)):
                    net.arrived(("xpm", dyl, s), xp.at[1 - core, gi(s, dyl)], mate)
    with jax.named_scope("xpt"):
        for t in range(4):
            xpt[:, 256 * t : 256 * t + 256] = jnp.transpose(
                xp[t // 2, pl.ds(8 * (t % 2), 8)].reshape(256, 896)
            )
    scoped("r_x13", r_x, 1, 3)
    scoped("r_last0", r_last, 0)
    scoped("weigh00", weigh, 0, 0)
    scoped("r_y1", r_y, 1)
    scoped("weigh01", weigh, 0, 1)
    scoped("r_x12", r_x, 1, 2)
    scoped("mix00", mix, 0, 0)
    scoped("mix01", mix, 0, 1)
    scoped("e_start0", e_start, 0)
    scoped("r_last1", r_last, 1)
    scoped("weigh10", weigh, 1, 0)
    scoped("weigh11", weigh, 1, 1)
    scoped("mix10", mix, 1, 0)
    scoped("mix11", mix, 1, 1)
    scoped("e_start1", e_start, 1)
    scoped("e_two0", e_two, 0)
    scoped("e_three0", e_three, 0)
    scoped("e_two1", e_two, 1)
    scoped("e_three1", e_three, 1)
    v0 = scoped("e_last0", e_last, 0)
    scoped("ladder0", ladder, 0, v0)
    v1 = scoped("e_last1", e_last, 1)
    scoped("ladder1", ladder, 1, v1)
    scoped("fold0", fold, 0)
    scoped("fold1", fold, 1)
    for k in range(2):
        total = fins[k]
        with jax.named_scope(f"f_wait{k}"):
            for dz in far:
                net.arrived(("f", k, dz), fr.at[k, dz], up(8 - dz))
                total = total + fr[k, dz].astype(F32)
        fins[k] = total
        net.start(("fin", k), fins.at[k], finr.at[k], mate)
    for k in range(2):
        out_ref[2 * core + k] = fins[k]
    with jax.named_scope("fin"):
        for k in range(2):
            net.arrived(("fin", k), finr.at[k], mate)
            out_ref[2 * (1 - core) + k] = finr[k]
    with jax.named_scope("close"):
        net.close()


def local(amplitudes, grid_factor, metric, virt_energy, pair_energy):
    core = lax.axis_index("blk") % 2
    t = jnp.pad(jnp.transpose(amplitudes, (1, 2, 0)), ((0, 0), (0, 8), (0, 8)))
    tt = jnp.concatenate([t[:, :32], t[:, 32:]], axis=2)
    vm = pl.BlockSpec(memory_space=pltpu.VMEM)
    out = pl.pallas_call(
        kernel,
        out_shape=jax.ShapeDtypeStruct((4, 64, 128), F32),
        in_specs=[vm, vm, pl.BlockSpec(memory_space=pltpu.HBM)],
        out_specs=vm,
        scratch_shapes=[
            pltpu.VMEM((2, 2, 16, 32, 128), BF16),
            pltpu.VMEM((8, 2, 32, 896), BF16),
            pltpu.VMEM((896, 512), BF16),
            pltpu.VMEM((2, 16, 32, 896), BF16),
            pltpu.VMEM((896, 1024), BF16),
            pltpu.VMEM((2, 512, 512), F32),
            pltpu.VMEM((2, 896, 512), BF16),
            pltpu.VMEM((1024, 512), BF16),
            pltpu.VMEM((2, 896, 512), F32),
            pltpu.VMEM((2, 3, 2, 48, 512), BF16),
            pltpu.VMEM((2, 3, 2, 48, 512), BF16),
            pltpu.VMEM((2, 3, 64, 512), BF16),
            pltpu.VMEM((2, 3, 64, 512), BF16),
            pltpu.VMEM((2, 48, 512), BF16),
            pltpu.VMEM((2, 48, 512), BF16),
            pltpu.VMEM((2, 4, 64, 512), BF16),
            pltpu.VMEM((2, 4, 64, 512), BF16),
            pltpu.VMEM((2, 896, 128), F32),
            pltpu.VMEM((2, 16, 64, 128), BF16),
            pltpu.VMEM((2, 8, 64, 128), BF16),
            pltpu.VMEM((2, 8, 64, 128), BF16),
            pltpu.VMEM((2, 64, 128), F32),
            pltpu.VMEM((2, 64, 128), F32),
            pltpu.SemaphoreType.DMA((SEMS,)),
            pltpu.SemaphoreType.DMA((SEMS,)),
            pltpu.SemaphoreType.DMA,
        ],
        compiler_params=pltpu.CompilerParams(
            collective_id=0, has_side_effects=True, vmem_limit_bytes=65000 * 1024
        ),
    )(tt, grid_factor, metric)
    ladder = jnp.where(core == 0, out[:, :56, :56], out[:, :56, 64:120])
    ladder = jnp.transpose(ladder, (2, 0, 1))
    rows, cols = amplitudes.shape[0], amplitudes.shape[2]
    first = lax.dynamic_slice_in_dim(virt_energy, lax.axis_index("blk") * rows, rows)
    second = lax.dynamic_slice_in_dim(virt_energy, lax.axis_index("grp") * cols, cols)
    denominator = first[:, None, None] + second[None, None, :] - pair_energy[None, :, None]
    return denominator * amplitudes.astype(F32) + ladder


def solution(mesh):
    in_specs = (P("blk", None, "grp"), P(("blk", "grp"), None), P("blk", "grp", None), P(), P())
    return jax.shard_map(
        local, mesh=mesh, in_specs=in_specs, out_specs=P("blk", None, "grp"), check_vma=False
    )
```

```python
import functools

import jax
import jax.numpy as jnp
from jax import lax
from jax.experimental import pallas as pl
from jax.experimental.pallas import tpu as pltpu
from jax.sharding import PartitionSpec as P

MESH = pl.DeviceIdType.MESH
F32 = jnp.float32
BF16 = jnp.bfloat16
SEMS = 200


class Links:
    def __init__(self, send, recv):
        self.send, self.recv, self.ids, self.open = send, recv, {}, []

    def index(self, key):
        assert len(self.ids) < SEMS
        return self.ids.setdefault(key, len(self.ids))

    def copy(self, key, src, dst, dev):
        i = self.index(key)
        return pltpu.make_async_remote_copy(
            src_ref=src, dst_ref=dst, send_sem=self.send.at[i], recv_sem=self.recv.at[i],
            device_id=dev, device_id_type=MESH,
        )

    def start(self, key, src, dst, dev):
        c = self.copy(key, src, dst, dev)
        c.start()
        self.open.append(c)

    def arrived(self, key, dst, dev):
        self.copy(key, dst, dst, dev).wait_recv()

    def close(self):
        for c in self.open:
            c.wait_send()
        self.open = []


def kernel(
    amp_hbm, x_hbm, z_hbm, ve_hbm, pe_hbm, out_ref,
    amp, x_ref, ve, pe, tt_ref, own_amp, base,
    tall, xq, xqt, xp, xpt, zb, right, w, mp,
    e1s, e1r, e2s, e2r, e3s, e3r, eys, eyr, lad, fs, fy, fr, fins, finr,
    send, recv, local_sem,
):
    b, g = lax.axis_index("blk"), lax.axis_index("grp")
    core, yh, x = b % 2, (b // 2) % 2, b // 4
    yl, z = g // 8, g % 8
    m = x * 2 + yh
    net = Links(send, recv)

    def at(dx, dy, dc=0):
        yy = 1 - yh if dy else yh
        cc = 1 - core if dc else core
        return {"blk": ((x + dx + 4) % 4) * 4 + yy * 2 + cc, "grp": g}

    def up(dz, dyl=0, dc=0):
        return {
            "blk": b + 1 - 2 * core if dc else b,
            "grp": ((1 - yl) if dyl else yl) * 8 + (z + dz) % 8,
        }

    mate, yp = at(0, 0, 1), at(0, 1)
    zn, zv, yn = up(1), up(7), up(0, 1)
    around = [(2, 1), (3, 1), (1, 1), (2, 0), (3, 0), (1, 0)]

    def rows(dx, o, first=0, count=112):
        yy = 1 - yh if o else yh
        return pl.ds(pl.multiple_of((((x + dx + 4) % 4) * 2 + yy) * 112 + first, 16), count)

    def xqa(dx, dy):
        return xq.at[((x + dx + 4) % 4) * 2 + ((1 - yh) if dy else yh), core]

    def gi(dz, dyl):
        return ((1 - yl) if dyl else yl) * 8 + (z + dz + 8) % 8

    def xpa(dyl, dz):
        return xp.at[core, gi(dz, dyl)]

    def fetch(i, src, dst):
        c = pltpu.make_async_copy(src, dst, local_sem.at[i])
        c.start()
        return c

    acopy, xcopy = fetch(0, amp_hbm, amp), fetch(1, x_hbm, x_ref)
    barrier = pltpu.get_barrier_semaphore()
    near = [mate, yn] + [at(dx, 0) for dx in range(1, 4)]
    near += [yp] + [up(dz, 0, dc) for dz in range(1, 8) for dc in range(2)]
    with jax.named_scope("barrier"):
        for dev in near:
            pl.semaphore_signal(barrier, inc=1, device_id=dev, device_id_type=MESH)
        vcopy, pcopy = fetch(2, ve_hbm, ve.at[pl.ds(0, 7)]), fetch(3, pe_hbm, pe)
        zcopy = fetch(4, z_hbm.at[:, 0, :], zb.at[core])
        acopy.wait()
        eye = (
            lax.broadcasted_iota(jnp.int32, (56, 64), 0)
            == lax.broadcasted_iota(jnp.int32, (56, 64), 1)
        ).astype(BF16)
        for k in range(4):
            t = lax.dot_general(
                amp[:, k, :], eye, (((0,), (0,)), ((), ())), preferred_element_type=F32
            )
            own_amp[k] = t
            t = jnp.concatenate([t, jnp.zeros((8, 64), F32)], axis=0)
            tt_ref[k] = jnp.concatenate([t[:32], t[32:]], axis=1).astype(BF16)
        xcopy.wait()
        pl.semaphore_wait(barrier, len(near))

    far = (4, 3, 5, 2, 6, 1, 7)

    def t_send(k):
        net.start(("t", k, 0, 1), tt_ref.at[2 * (1 - core) + k], tall.at[k, core, g], mate)
        for dz in far:
            for dc in range(2):
                pair = 2 * ((1 - core) if dc else core) + k
                net.start(("t", k, dz, dc), tt_ref.at[pair], tall.at[k, core, g], up(dz, 0, dc))
        tall[k, core, g] = tt_ref[2 * core + k]

    def t_forward(k, dz):
        j = gi(-dz, 0)
        for dc in range(2):
            if dz or dc:
                part = tall.at[k, (1 - core) if dc else core, j]
                net.arrived(("t", k, dz, dc), part, up(8 - dz, 0, dc))
        net.start(("ty", k, dz), tall.at[k, :, j], tall.at[k, :, j], yn)

    t_send(0)
    net.start("xpy", x_ref, xpa(0, 0), yn)
    for dx, dy in ((0, 1), (1, 0), (3, 0), (2, 0)):
        net.start(("xq", dx, dy), x_ref, xqa(0, 0), at(dx, dy))
    net.start(("xqm", 0, 0), x_ref, xqa(0, 0), mate)
    net.start(("xpn", 0, 1), x_ref, xpa(0, 0), zn)
    net.start(("xpv", 0, 1), x_ref, xpa(0, 0), zv)
    net.start(("xpm", 0, 0), x_ref, xpa(0, 0), mate)
    xq[m, core] = x_ref[...]
    xp[core, g] = x_ref[...]

    def xq_forward(dx, dy):
        part = xqa(-dx, dy)
        net.arrived(("xq", dx, dy), part, at(4 - dx, 0 if dx else dy))
        if (dx, dy) == (0, 1):
            for to in (1, 3, 2):
                net.start(("xq", to, 1), part, part, at(to, 0))
        net.start(("xqm", dx, dy), part, part, mate)

    lane = lax.broadcasted_iota(jnp.int32, (512, 128), 1)

    def first(k):
        for dz in (0,) + far:
            net.arrived(("ty", k, dz), tall.at[k, :, gi(-dz, 1)], yn)
        one = tall[k, 0].reshape(512, 128).astype(F32)
        two = tall[k, 1].reshape(512, 128).astype(F32)
        top = jnp.where(lane < 64, one, pltpu.roll(two, 64, 1))
        low = jnp.where(lane < 64, pltpu.roll(one, 64, 1), two)
        t = jnp.concatenate(
            [v for j in range(16) for v in (top[32 * j : 32 * j + 32], low[32 * j : 32 * j + 24])],
            axis=0,
        )
        rt = lax.dot_general(
            t.astype(BF16), xq[...].reshape(512, 896), (((0,), (1,)), ((), ())),
            preferred_element_type=F32,
        )
        right[k, rows(0, 0)] = jnp.concatenate([rt[:56], rt[64:120]], axis=0).astype(BF16)
        own = right.at[k, rows(0, 0)]
        net.start(("ry", k, 0), own, own, yp)
        for dx in (1, 3, 2):
            net.start(("rx", k, dx), own, own, at(dx, 0))

    def xp_mate(dyl, dz):
        net.start(("xpm", dyl, dz), xpa(dyl, dz), xpa(dyl, dz), mate)

    def xp_y():
        part = xpa(1, 0)
        net.arrived("xpy", part, yn)
        net.start(("xpn", 1, 1), part, part, zn)
        net.start(("xpv", 1, 1), part, part, zv)
        xp_mate(1, 0)

    def xp_step(s, dyl):
        if s < 4 or dyl == 0:
            part = xpa(dyl, -s)
            net.arrived(("xpn", dyl, s), part, zv)
            if s < 3 or (s == 3 and dyl == 0):
                net.start(("xpn", dyl, s + 1), part, part, zn)
            xp_mate(dyl, -s)
        if s < 4 or dyl == 1:
            part = xpa(dyl, s)
            net.arrived(("xpv", dyl, s), part, zn)
            if s < 3 or (s == 3 and dyl == 1):
                net.start(("xpv", dyl, s + 1), part, part, zv)
            xp_mate(dyl, s)

    def r_y(k):
        net.arrived(("ry", k, 0), right.at[k, rows(0, 1)], yp)
        part = right.at[k, rows(0, 1, 0, 48)]
        for dx in (1, 3, 2):
            net.start(("rz", k, dx), part, part, at(dx, 0))

    def r_x(k, *ways):
        for dx in ways:
            net.arrived(("rx", k, dx), right.at[k, rows(-dx, 0)], at(4 - dx, 0))
            part = right.at[k, rows(-dx, 0, 48, 64)]
            net.start(("ry", k, dx), part, part, yp)

    def r_last(k):
        for dx in (1, 3, 2):
            net.arrived(("rz", k, dx), right.at[k, rows(-dx, 1, 0, 48)], at(4 - dx, 0))
        for dx in (1, 3, 2):
            net.arrived(("ry", k, dx), right.at[k, rows(-dx, 1, 48, 64)], yp)

    def weigh(k, c):
        p = jnp.dot(xp[c].reshape(512, 896), right[k], preferred_element_type=F32)
        w[512 * c : 512 * c + 512, :] = (zb[c] * p).astype(BF16)

    def mix(k, t):
        a = pl.ds(448 * t, 448)
        mp[k, a, :] = jnp.dot(xpt[a, :], w[...], preferred_element_type=F32)

    order = (2, 1, 3, 0)

    def e_start(k):
        for i, dx in enumerate(order):
            eys[k, i] = mp[k, rows(dx, 1, 48, 64), :].astype(BF16)
            net.start(("ey", k, dx), eys.at[k, i], eyr.at[k, i], yp)
            if dx:
                for o in range(2):
                    e1s[k, i, o] = mp[k, rows(dx, o, 0, 48), :].astype(BF16)
                net.start(("e1", k, dx), e1s.at[k, i], e1r.at[k, i], at(dx, 0))

    def e_y(k, dx):
        i = order.index(dx)
        net.arrived(("ey", k, dx), eyr.at[k, i], yp)
        return mp[k, rows(dx, 0, 48, 64), :] + eyr[k, i].astype(F32)

    def e_two(k):
        for i, dx in enumerate(order[:3]):
            e2s[k, i] = e_y(k, dx).astype(BF16)
            net.start(("e2", k, dx), e2s.at[k, i], e2r.at[k, i], at(dx, 0))

    def e_three(k):
        v = mp[k, rows(0, 1, 0, 48), :]
        for i, dx in enumerate(order[:3]):
            net.arrived(("e1", k, dx), e1r.at[k, i], at(4 - dx, 0))
            v = v + e1r[k, i, 1].astype(F32)
        e3s[k] = v.astype(BF16)
        net.start(("e3", k), e3s.at[k], e3r.at[k], yp)

    def e_last(k):
        v = e_y(k, 0)
        for i, dx in enumerate(order[:3]):
            net.arrived(("e2", k, dx), e2r.at[k, i], at(4 - dx, 0))
            v = v + e2r[k, i].astype(F32)
        u = mp[k, rows(0, 0, 0, 48), :]
        for i in range(3):
            u = u + e1r[k, i, 0].astype(F32)
        net.arrived(("e3", k), e3r.at[k], yp)
        return jnp.concatenate([u + e3r[k].astype(F32), v], axis=0)

    def ladder(k, v):
        gap = jnp.zeros((8, 512), F32)
        v = jnp.concatenate([v[:56], gap, v[56:], gap], axis=0).astype(BF16)
        lad[k] = lax.dot_general(
            xqt[...], v, (((1,), (1,)), ((), ())), preferred_element_type=F32
        )
        gap = jnp.zeros((8, 128), F32)
        for dz in range(8):
            j = gi(dz, 1)
            v = lad[k, pl.ds(pl.multiple_of(j * 56, 8), 56), :]
            fs[k, j] = jnp.concatenate([v, gap], axis=0).astype(BF16)
        for dz in far + (0,):
            net.start(("fy", k, dz), fs.at[k, gi(dz, 1)], fy.at[k, dz], yn)

    def fold(k):
        for dz in far + (0,):
            j = gi(dz, 0)
            net.arrived(("fy", k, dz), fy.at[k, dz], yn)
            v = lad[k, pl.ds(pl.multiple_of(j * 56, 8), 56), :] + fy[k, dz, 0:56].astype(F32)
            v = jnp.concatenate([v, jnp.zeros((8, 128), F32)], axis=0)
            if dz:
                fs[k, j] = v.astype(BF16)
                net.start(("f", k, dz), fs.at[k, j], fr.at[k, dz], up(dz))
            else:
                fins[k] = v

    def scoped(name, f, *args):
        with jax.named_scope(name):
            return f(*args)

    scoped("xp_y", xp_y)
    scoped("xq_y", xq_forward, 0, 1)
    with jax.named_scope("t0_xq"):
        t_forward(0, 0)
        for i, dz in enumerate(far[::-1]):
            t_forward(0, dz)
            if i < 3:
                xq_forward(*around[::-1][i])
    scoped("xp_step10", xp_step, 1, 0)
    scoped("xp_step11", xp_step, 1, 1)
    t_send(1)
    with jax.named_scope("xq_far"):
        for dx, dy in around[2::-1]:
            xq_forward(dx, dy)
    with jax.named_scope("xqm_wait"):
        for dx, dy in around + [(0, 1), (0, 0)]:
            part = xq.at[((x - dx + 4) % 4) * 2 + ((1 - yh) if dy else yh), 1 - core]
            net.arrived(("xqm", dx, dy), part, mate)
    scoped("first0", first, 0)
    scoped("xp_step20", xp_step, 2, 0)
    scoped("xp_step21", xp_step, 2, 1)
    with jax.named_scope("xqt"):
        xqt[...] = jnp.transpose(xq[...].reshape(512, 896))
    with jax.named_scope("energies"):
        vcopy.wait()
        pcopy.wait()

        def run(start):
            r, off = start // 128, start % 128
            lane = lax.broadcasted_iota(jnp.int32, (8, 128), 1)
            one = jnp.broadcast_to(ve[pl.ds(r, 1), :], (8, 128))
            two = jnp.broadcast_to(ve[pl.ds(jnp.minimum(r + 1, 6), 1), :], (8, 128))
            shift = (128 - off) % 128
            return jnp.where(lane < 128 - off, pltpu.roll(one, shift, 1), pltpu.roll(two, shift, 1))

        first_e = run(b * 56)[0:1, :64]
        second_e = jnp.transpose(jnp.broadcast_to(run(g * 56)[0:1], (128, 128)))[:56, :64]
        both = second_e + first_e
        for k in range(4):
            base[k] = (both - pe[k]) * own_amp[k]
    net.start("zsw", z_hbm.at[:, 0, :], zb.at[core], mate)
    with jax.named_scope("t1"):
        for dz in (0,) + far[::-1]:
            t_forward(1, dz)
    scoped("r_x01", r_x, 0, 1)
    scoped("xp_step30", xp_step, 3, 0)
    scoped("r_x03", r_x, 0, 3)
    scoped("xp_step31", xp_step, 3, 1)
    scoped("r_y0", r_y, 0)
    scoped("r_x02", r_x, 0, 2)
    scoped("first1", first, 1)
    scoped("xp_step40", xp_step, 4, 0)
    scoped("xp_step41", xp_step, 4, 1)
    with jax.named_scope("z_wait"):
        zcopy.wait()
        net.arrived("zsw", zb.at[1 - core], mate)
    with jax.named_scope("xpm_wait"):
        for s in range(-4, 5):
            for dyl in range(2):
                if (s, dyl) not in ((4, 0), (-4, 1)):
                    net.arrived(("xpm", dyl, s), xp.at[1 - core, gi(s, dyl)], mate)
    with jax.named_scope("xpt"):
        for t in range(4):
            xpt[:, 256 * t : 256 * t + 256] = jnp.transpose(
                xp[t // 2, pl.ds(8 * (t % 2), 8)].reshape(256, 896)
            )
    scoped("r_last0", r_last, 0)
    scoped("weigh00", weigh, 0, 0)
    scoped("r_x11", r_x, 1, 1)
    scoped("r_x13", r_x, 1, 3)
    scoped("r_y1", r_y, 1)
    scoped("weigh01", weigh, 0, 1)
    scoped("r_x12", r_x, 1, 2)
    scoped("mix00", mix, 0, 0)
    scoped("mix01", mix, 0, 1)
    scoped("e_start0", e_start, 0)
    scoped("r_last1", r_last, 1)
    scoped("weigh10", weigh, 1, 0)
    scoped("weigh11", weigh, 1, 1)
    scoped("mix10", mix, 1, 0)
    scoped("mix11", mix, 1, 1)
    scoped("e_start1", e_start, 1)
    scoped("e_two0", e_two, 0)
    scoped("e_three0", e_three, 0)
    scoped("e_two1", e_two, 1)
    scoped("e_three1", e_three, 1)
    v0 = scoped("e_last0", e_last, 0)
    scoped("ladder0", ladder, 0, v0)
    v1 = scoped("e_last1", e_last, 1)
    scoped("ladder1", ladder, 1, v1)
    scoped("fold0", fold, 0)
    scoped("fold1", fold, 1)
    scoped("close1", net.close)
    for k in range(2):
        total = fins[k]
        with jax.named_scope(f"f_wait{k}"):
            for dz in far:
                net.arrived(("f", k, dz), fr.at[k, dz], up(8 - dz))
                total = total + fr[k, dz].astype(F32)
        fins[k] = total
        net.start(("fin", k), fins.at[k], finr.at[k], mate)
    def finish(pair, v):
        v = jnp.where(core == 0, v[:56, :64], v[:56, 64:]) + base[pair]
        out_ref[pair] = v[:, :56]

    for k in range(2):
        finish(2 * core + k, fins[k])
    with jax.named_scope("fin"):
        for k in range(2):
            net.arrived(("fin", k), finr.at[k], mate)
            finish(2 * (1 - core) + k, finr[k])
    with jax.named_scope("close"):
        net.close()


def local(amplitudes, grid_factor, metric, virt_energy, pair_energy):
    rows, pairs, cols = amplitudes.shape
    hbm = pl.BlockSpec(memory_space=pltpu.HBM)
    out = pl.pallas_call(
        kernel,
        out_shape=jax.ShapeDtypeStruct((pairs, cols, rows), F32),
        in_specs=[hbm] * 5,
        out_specs=pl.BlockSpec(memory_space=pltpu.VMEM),
        scratch_shapes=[
            pltpu.VMEM((56, 4, 56), BF16),
            pltpu.VMEM((32, 896), BF16),
            pltpu.VMEM((8, 128), F32),
            pltpu.SMEM((4,), F32),
            pltpu.VMEM((4, 32, 128), BF16),
            pltpu.VMEM((4, 56, 64), F32),
            pltpu.VMEM((4, 56, 64), F32),
            pltpu.VMEM((2, 2, 16, 32, 128), BF16),
            pltpu.VMEM((8, 2, 32, 896), BF16),
            pltpu.VMEM((896, 512), BF16),
            pltpu.VMEM((2, 16, 32, 896), BF16),
            pltpu.VMEM((896, 1024), BF16),
            pltpu.VMEM((2, 512, 512), F32),
            pltpu.VMEM((2, 896, 512), BF16),
            pltpu.VMEM((1024, 512), BF16),
            pltpu.VMEM((2, 896, 512), F32),
            pltpu.VMEM((2, 3, 2, 48, 512), BF16),
            pltpu.VMEM((2, 3, 2, 48, 512), BF16),
            pltpu.VMEM((2, 3, 64, 512), BF16),
            pltpu.VMEM((2, 3, 64, 512), BF16),
            pltpu.VMEM((2, 48, 512), BF16),
            pltpu.VMEM((2, 48, 512), BF16),
            pltpu.VMEM((2, 4, 64, 512), BF16),
            pltpu.VMEM((2, 4, 64, 512), BF16),
            pltpu.VMEM((2, 896, 128), F32),
            pltpu.VMEM((2, 16, 64, 128), BF16),
            pltpu.VMEM((2, 8, 64, 128), BF16),
            pltpu.VMEM((2, 8, 64, 128), BF16),
            pltpu.VMEM((2, 64, 128), F32),
            pltpu.VMEM((2, 64, 128), F32),
            pltpu.SemaphoreType.DMA((SEMS,)),
            pltpu.SemaphoreType.DMA((SEMS,)),
            pltpu.SemaphoreType.DMA((5,)),
        ],
        compiler_params=pltpu.CompilerParams(
            collective_id=0, has_side_effects=True, vmem_limit_bytes=65000 * 1024
        ),
    )(amplitudes, grid_factor, metric, virt_energy.reshape(7, 128), pair_energy)
    return jnp.transpose(out, (2, 0, 1))


def solution(mesh):
    in_specs = (P("blk", None, "grp"), P(("blk", "grp"), None), P("blk", "grp", None), P(), P())
    return jax.shard_map(
        local, mesh=mesh, in_specs=in_specs, out_specs=P("blk", None, "grp"), check_vma=False
    )
```

```python
import functools

import jax
import jax.numpy as jnp
from jax import lax
from jax.experimental import pallas as pl
from jax.experimental.pallas import tpu as pltpu
from jax.sharding import PartitionSpec as P

MESH = pl.DeviceIdType.MESH
F32 = jnp.float32
BF16 = jnp.bfloat16
NAMES, KINDS = 89, 15


class Links:
    def __init__(self, send, recv):
        self.send, self.recv, self.ids, self.kinds = send, recv, {}, {}

    def index(self, names, name, most):
        assert name in names or len(names) < most
        return names.setdefault(name, len(names))

    def copy(self, kind, name, src, dst, dev):
        return pltpu.make_async_remote_copy(
            src_ref=src, dst_ref=dst,
            send_sem=self.send.at[self.index(self.kinds, kind, KINDS)],
            recv_sem=self.recv.at[self.index(self.ids, name, NAMES)],
            device_id=dev, device_id_type=MESH,
        )

    def start(self, kind, name, src, dst, dev):
        self.copy(kind, name, src, dst, dev).start()

    def arrived(self, name, dst, dev):
        i = self.index(self.ids, name, NAMES)
        pltpu.make_async_remote_copy(
            src_ref=dst, dst_ref=dst, send_sem=self.send.at[0], recv_sem=self.recv.at[i],
            device_id=dev, device_id_type=MESH,
        ).wait_recv()

    def sent(self, kind, all_of_them, dev):
        pltpu.make_async_remote_copy(
            src_ref=all_of_them, dst_ref=all_of_them, send_sem=self.send.at[self.kinds[kind]],
            recv_sem=self.recv.at[0], device_id=dev, device_id_type=MESH,
        ).wait_send()


def kernel(
    amp_hbm, x_hbm, z_hbm, ve_hbm, pe_hbm, out_ref,
    amp, x_ref, ve, pe, tt_ref, own_amp, base,
    tall, xq, xqt, xp, xpt, zb, right, w, mp,
    e1s, e1r, e2s, e2r, e3s, e3r, eys, eyr, lad, fs, fy, fr, fins, finr,
    send, recv, local_sem,
):
    b, g = lax.axis_index("blk"), lax.axis_index("grp")
    core, yh, x = b % 2, (b // 2) % 2, b // 4
    yl, z = g // 8, g % 8
    m = x * 2 + yh
    net = Links(send, recv)

    def at(dx, dy, dc=0):
        yy = 1 - yh if dy else yh
        cc = 1 - core if dc else core
        return {"blk": ((x + dx + 4) % 4) * 4 + yy * 2 + cc, "grp": g}

    def up(dz, dyl=0, dc=0):
        return {
            "blk": b + 1 - 2 * core if dc else b,
            "grp": ((1 - yl) if dyl else yl) * 8 + (z + dz) % 8,
        }

    mate, xn, yp = at(0, 0, 1), at(1, 0), at(0, 1)
    zn, zv, yn = up(1), up(7), up(0, 1)
    around = [(2, 1), (3, 1), (1, 1), (2, 0), (3, 0), (1, 0)]

    def rows(dx, o, first=0, count=112):
        yy = 1 - yh if o else yh
        return pl.ds(pl.multiple_of((((x + dx + 4) % 4) * 2 + yy) * 112 + first, 16), count)

    def xqa(dx, dy):
        return xq.at[((x + dx + 4) % 4) * 2 + ((1 - yh) if dy else yh), core]

    def gi(dz, dyl):
        return ((1 - yl) if dyl else yl) * 8 + (z + dz + 8) % 8

    def xpa(dyl, dz):
        return xp.at[core, gi(dz, dyl)]

    def fetch(i, src, dst):
        c = pltpu.make_async_copy(src, dst, local_sem.at[i])
        c.start()
        return c

    acopy, xcopy = fetch(0, amp_hbm, amp), fetch(1, x_hbm, x_ref)
    barrier = pltpu.get_barrier_semaphore()
    near = [mate, yn] + [at(dx, 0) for dx in range(1, 4)]
    near += [yp] + [up(dz, 0, dc) for dz in range(1, 8) for dc in range(2)]
    with jax.named_scope("barrier"):
        for dev in near:
            pl.semaphore_signal(barrier, inc=1, device_id=dev, device_id_type=MESH)
        vcopy, pcopy = fetch(2, ve_hbm, ve.at[pl.ds(0, 7)]), fetch(3, pe_hbm, pe)
        zcopy = fetch(4, z_hbm.at[:, 0, :], zb.at[core])
        acopy.wait()
        eye = (
            lax.broadcasted_iota(jnp.int32, (56, 64), 0)
            == lax.broadcasted_iota(jnp.int32, (56, 64), 1)
        ).astype(BF16)
        for k in range(4):
            t = lax.dot_general(
                amp[:, k, :], eye, (((0,), (0,)), ((), ())), preferred_element_type=F32
            )
            own_amp[k] = t
            t = jnp.concatenate([t, jnp.zeros((8, 64), F32)], axis=0)
            tt_ref[k] = jnp.concatenate([t[:32], t[32:]], axis=1).astype(BF16)
        xcopy.wait()
        pl.semaphore_wait(barrier, len(near))

    far = (4, 3, 5, 2, 6, 1, 7)

    def t_send(k):
        net.start("t", ("t", k, 0), tt_ref.at[2 * (1 - core) + k], tall.at[k, core, g], mate)
        for dz in far:
            for dc in range(2):
                pair = 2 * ((1 - core) if dc else core) + k
                net.start("t", ("t", k, dz), tt_ref.at[pair], tall.at[k, core, g], up(dz, 0, dc))
        tall[k, core, g] = tt_ref[2 * core + k]

    def t_forward(k, dz):
        j = gi(-dz, 0)
        if dz:
            net.arrived(("t", k, dz), tall.at[k, :, j], up(8 - dz))
        else:
            net.arrived(("t", k, dz), tall.at[k, 1 - core, j], mate)
        net.start("ty", ("ty", k), tall.at[k, :, j], tall.at[k, :, j], yn)

    t_send(0)
    net.start("x", "xpy", x_ref, xpa(0, 0), yn)
    for dx, dy in ((0, 1), (1, 0), (3, 0), (2, 0)):
        net.start("x", ("xq", dx, dy), x_ref, xqa(0, 0), at(dx, dy))
    net.start("x", "xqm", x_ref, xqa(0, 0), mate)
    net.start("xp", ("xpn", 0, 1), x_ref, xpa(0, 0), zn)
    net.start("xp", ("xpv", 0, 1), x_ref, xpa(0, 0), zv)
    net.start("xpm", "xpm", x_ref, xpa(0, 0), mate)
    xq[m, core] = x_ref[...]
    xp[core, g] = x_ref[...]

    def xq_forward(dx, dy):
        part = xqa(-dx, dy)
        net.arrived(("xq", dx, dy), part, at(4 - dx, 0 if dx else dy))
        if (dx, dy) == (0, 1):
            for to in (1, 3, 2):
                net.start("x", ("xq", to, 1), part, part, at(to, 0))
        net.start("x", "xqm", part, part, mate)

    lane = lax.broadcasted_iota(jnp.int32, (512, 128), 1)

    def first(k):
        net.arrived(("ty", k), tall.at[k, :, pl.ds(8 * (1 - yl), 8)], yn)
        one = tall[k, 0].reshape(512, 128).astype(F32)
        two = tall[k, 1].reshape(512, 128).astype(F32)
        top = jnp.where(lane < 64, one, pltpu.roll(two, 64, 1))
        low = jnp.where(lane < 64, pltpu.roll(one, 64, 1), two)
        t = jnp.concatenate(
            [v for j in range(16) for v in (top[32 * j : 32 * j + 32], low[32 * j : 32 * j + 24])],
            axis=0,
        )
        rt = lax.dot_general(
            t.astype(BF16), xq[...].reshape(512, 896), (((0,), (1,)), ((), ())),
            preferred_element_type=F32,
        )
        right[k, rows(0, 0)] = jnp.concatenate([rt[:56], rt[64:120]], axis=0).astype(BF16)
        own = right.at[k, rows(0, 0)]
        net.start("r", ("ry", k), own, own, yp)
        for dx in (1, 3, 2):
            net.start("r", ("rx", k, dx), own, own, at(dx, 0))

    def xp_mate(dyl, dz):
        net.start("xpm", "xpm", xpa(dyl, dz), xpa(dyl, dz), mate)

    def xp_y():
        part = xpa(1, 0)
        net.arrived("xpy", part, yn)
        net.start("xp", ("xpn", 1, 1), part, part, zn)
        net.start("xp", ("xpv", 1, 1), part, part, zv)
        xp_mate(1, 0)

    def xp_step(s, dyl):
        if s < 4 or dyl == 0:
            part = xpa(dyl, -s)
            net.arrived(("xpn", dyl, s), part, zv)
            if s < 3 or (s == 3 and dyl == 0):
                net.start("xp", ("xpn", dyl, s + 1), part, part, zn)
            xp_mate(dyl, -s)
        if s < 4 or dyl == 1:
            part = xpa(dyl, s)
            net.arrived(("xpv", dyl, s), part, zn)
            if s < 3 or (s == 3 and dyl == 1):
                net.start("xp", ("xpv", dyl, s + 1), part, part, zv)
            xp_mate(dyl, s)

    def r_y(k):
        net.arrived(("ry", k), right.at[k, rows(0, 1)], yp)
        part = right.at[k, rows(0, 1, 0, 48)]
        for dx in (1, 3, 2):
            net.start("r2", ("rz", k), part, part, at(dx, 0))

    def r_x(k, *ways):
        for dx in ways:
            net.arrived(("rx", k, dx), right.at[k, rows(-dx, 0)], at(4 - dx, 0))
            part = right.at[k, rows(-dx, 0, 48, 64)]
            net.start("r2", ("rw", k), part, part, yp)

    def r_last(k):
        net.arrived(("rz", k), right.at[k, pl.ds(0, 144)], xn)
        net.arrived(("rw", k), right.at[k, pl.ds(0, 192)], yp)

    def weigh(k, c):
        p = jnp.dot(xp[c].reshape(512, 896), right[k], preferred_element_type=F32)
        w[512 * c : 512 * c + 512, :] = (zb[c] * p).astype(BF16)

    def mix(k, t):
        a = pl.ds(448 * t, 448)
        mp[k, a, :] = jnp.dot(xpt[a, :], w[...], preferred_element_type=F32)

    order = (2, 1, 3, 0)

    def e_start(k):
        for i, dx in enumerate(order):
            eys[k, i] = mp[k, rows(dx, 1, 48, 64), :].astype(BF16)
            net.start("ey", ("ey", k, dx), eys.at[k, i], eyr.at[k, i], yp)
            if dx:
                for o in range(2):
                    e1s[k, i, o] = mp[k, rows(dx, o, 0, 48), :].astype(BF16)
                net.start("e1", ("e1", k), e1s.at[k, i], e1r.at[k, i], at(dx, 0))

    def e_y(k, dx):
        i = order.index(dx)
        net.arrived(("ey", k, dx), eyr.at[k, i], yp)
        return mp[k, rows(dx, 0, 48, 64), :] + eyr[k, i].astype(F32)

    def e_two(k):
        for i, dx in enumerate(order[:3]):
            e2s[k, i] = e_y(k, dx).astype(BF16)
            net.start("e2", ("e2", k), e2s.at[k, i], e2r.at[k, i], at(dx, 0))

    def e_three(k):
        v = mp[k, rows(0, 1, 0, 48), :]
        net.arrived(("e1", k), e1r.at[k], xn)
        for i in range(3):
            v = v + e1r[k, i, 1].astype(F32)
        e3s[k] = v.astype(BF16)
        net.start("e3", ("e3", k), e3s.at[k], e3r.at[k], yp)

    def e_last(k):
        v = e_y(k, 0)
        net.arrived(("e2", k), e2r.at[k], xn)
        for i in range(3):
            v = v + e2r[k, i].astype(F32)
        u = mp[k, rows(0, 0, 0, 48), :]
        for i in range(3):
            u = u + e1r[k, i, 0].astype(F32)
        net.arrived(("e3", k), e3r.at[k], yp)
        return jnp.concatenate([u + e3r[k].astype(F32), v], axis=0)

    def ladder(k, v):
        gap = jnp.zeros((8, 512), F32)
        v = jnp.concatenate([v[:56], gap, v[56:], gap], axis=0).astype(BF16)
        lad[k] = lax.dot_general(
            xqt[...], v, (((1,), (1,)), ((), ())), preferred_element_type=F32
        )
        gap = jnp.zeros((8, 128), F32)
        for dz in range(8):
            j = gi(dz, 1)
            v = lad[k, pl.ds(pl.multiple_of(j * 56, 8), 56), :]
            fs[k, j] = jnp.concatenate([v, gap], axis=0).astype(BF16)
        for dz in far + (0,):
            net.start("fy", ("fy", k, dz), fs.at[k, gi(dz, 1)], fy.at[k, dz], yn)

    def fold(k):
        for dz in far + (0,):
            j = gi(dz, 0)
            net.arrived(("fy", k, dz), fy.at[k, dz], yn)
            v = lad[k, pl.ds(pl.multiple_of(j * 56, 8), 56), :] + fy[k, dz, 0:56].astype(F32)
            v = jnp.concatenate([v, jnp.zeros((8, 128), F32)], axis=0)
            if dz:
                fs[k, j] = v.astype(BF16)
                net.start("f", ("f", k), fs.at[k, j], fr.at[k, dz], up(dz))
            else:
                fins[k] = v

    def scoped(name, f, *args):
        with jax.named_scope(name):
            return f(*args)

    scoped("xp_y", xp_y)
    scoped("xq_y", xq_forward, 0, 1)
    with jax.named_scope("t0_xq"):
        t_forward(0, 0)
        for i, dz in enumerate(far[::-1]):
            t_forward(0, dz)
            if i < 3:
                xq_forward(*around[::-1][i])
    scoped("xp_step10", xp_step, 1, 0)
    scoped("xp_step11", xp_step, 1, 1)
    t_send(1)
    with jax.named_scope("xq_far"):
        for dx, dy in around[2::-1]:
            xq_forward(dx, dy)
    with jax.named_scope("xqm_wait"):
        net.arrived("xqm", xq.at[:, 1 - core], mate)
    scoped("first0", first, 0)
    scoped("xp_step20", xp_step, 2, 0)
    scoped("xp_step21", xp_step, 2, 1)
    with jax.named_scope("xqt"):
        xqt[...] = jnp.transpose(xq[...].reshape(512, 896))
    with jax.named_scope("energies"):
        vcopy.wait()
        pcopy.wait()

        def run(start):
            r, off = start // 128, start % 128
            lane = lax.broadcasted_iota(jnp.int32, (8, 128), 1)
            one = jnp.broadcast_to(ve[pl.ds(r, 1), :], (8, 128))
            two = jnp.broadcast_to(ve[pl.ds(jnp.minimum(r + 1, 6), 1), :], (8, 128))
            shift = (128 - off) % 128
            return jnp.where(lane < 128 - off, pltpu.roll(one, shift, 1), pltpu.roll(two, shift, 1))

        first_e = run(b * 56)[0:1, :64]
        second_e = jnp.transpose(jnp.broadcast_to(run(g * 56)[0:1], (128, 128)))[:56, :64]
        both = second_e + first_e
        for k in range(4):
            base[k] = (both - pe[k]) * own_amp[k]
    net.start("z", "z", z_hbm.at[:, 0, :], zb.at[core], mate)
    with jax.named_scope("t1"):
        for dz in (0,) + far[::-1]:
            t_forward(1, dz)
    scoped("r_x01", r_x, 0, 1)
    scoped("xp_step30", xp_step, 3, 0)
    scoped("r_x03", r_x, 0, 3)
    scoped("xp_step31", xp_step, 3, 1)
    scoped("r_y0", r_y, 0)
    scoped("r_x02", r_x, 0, 2)
    scoped("first1", first, 1)
    scoped("xp_step40", xp_step, 4, 0)
    scoped("xp_step41", xp_step, 4, 1)
    with jax.named_scope("z_wait"):
        zcopy.wait()
        net.arrived("z", zb.at[1 - core], mate)
    with jax.named_scope("xpm_wait"):
        net.arrived("xpm", xp.at[1 - core], mate)
    with jax.named_scope("xpt"):
        for t in range(4):
            xpt[:, 256 * t : 256 * t + 256] = jnp.transpose(
                xp[t // 2, pl.ds(8 * (t % 2), 8)].reshape(256, 896)
            )
    scoped("r_last0", r_last, 0)
    scoped("weigh00", weigh, 0, 0)
    scoped("r_x11", r_x, 1, 1)
    scoped("r_x13", r_x, 1, 3)
    scoped("r_y1", r_y, 1)
    scoped("weigh01", weigh, 0, 1)
    scoped("r_x12", r_x, 1, 2)
    scoped("mix00", mix, 0, 0)
    scoped("mix01", mix, 0, 1)
    scoped("e_start0", e_start, 0)
    scoped("r_last1", r_last, 1)
    scoped("weigh10", weigh, 1, 0)
    scoped("weigh11", weigh, 1, 1)
    scoped("mix10", mix, 1, 0)
    scoped("mix11", mix, 1, 1)
    scoped("e_start1", e_start, 1)
    scoped("e_two0", e_two, 0)
    scoped("e_three0", e_three, 0)
    scoped("e_two1", e_two, 1)
    scoped("e_three1", e_three, 1)
    v0 = scoped("e_last0", e_last, 0)
    scoped("ladder0", ladder, 0, v0)
    v1 = scoped("e_last1", e_last, 1)
    scoped("ladder1", ladder, 1, v1)
    scoped("fold0", fold, 0)
    scoped("fold1", fold, 1)
    for k in range(2):
        total = fins[k]
        with jax.named_scope(f"f_wait{k}"):
            net.arrived(("f", k), fr.at[k, pl.ds(1, 7)], zn)
            for dz in far:
                total = total + fr[k, dz].astype(F32)
        fins[k] = total
        net.start("fin", ("fin", k), fins.at[k], finr.at[k], mate)
    def finish(pair, v):
        v = jnp.where(core == 0, v[:56, :64], v[:56, 64:]) + base[pair]
        out_ref[pair] = v[:, :56]

    for k in range(2):
        finish(2 * core + k, fins[k])
    with jax.named_scope("fin"):
        for k in range(2):
            net.arrived(("fin", k), finr.at[k], mate)
            finish(2 * (1 - core) + k, finr[k])
    with jax.named_scope("close"):
        for kind, whole in (
            ("t", tall.at[:, 0, pl.ds(0, 15)]), ("ty", tall.at[:, 0]), ("x", xq),
            ("xp", xp.at[0, pl.ds(0, 14)]), ("xpm", xp.at[0]), ("z", zb.at[0]),
            ("r", right.at[0]), ("r2", right.at[0, pl.ds(0, 672)]), ("ey", eys), ("e1", e1s),
            ("e2", e2s), ("e3", e3s), ("fy", fy), ("f", fr.at[:, pl.ds(0, 7)]), ("fin", fins),
        ):
            net.sent(kind, whole, mate)


def local(amplitudes, grid_factor, metric, virt_energy, pair_energy):
    rows, pairs, cols = amplitudes.shape
    hbm = pl.BlockSpec(memory_space=pltpu.HBM)
    out = pl.pallas_call(
        kernel,
        out_shape=pltpu.VMEM((pairs, cols, rows), F32),
        in_specs=[hbm] * 5,
        out_specs=pl.BlockSpec(memory_space=pltpu.VMEM),
        scratch_shapes=[
            pltpu.VMEM((56, 4, 56), BF16),
            pltpu.VMEM((32, 896), BF16),
            pltpu.VMEM((8, 128), F32),
            pltpu.SMEM((4,), F32),
            pltpu.VMEM((4, 32, 128), BF16),
            pltpu.VMEM((4, 56, 64), F32),
            pltpu.VMEM((4, 56, 64), F32),
            pltpu.VMEM((2, 2, 16, 32, 128), BF16),
            pltpu.VMEM((8, 2, 32, 896), BF16),
            pltpu.VMEM((896, 512), BF16),
            pltpu.VMEM((2, 16, 32, 896), BF16),
            pltpu.VMEM((896, 1024), BF16),
            pltpu.VMEM((2, 512, 512), F32),
            pltpu.VMEM((2, 896, 512), BF16),
            pltpu.VMEM((1024, 512), BF16),
            pltpu.VMEM((2, 896, 512), F32),
            pltpu.VMEM((2, 3, 2, 48, 512), BF16),
            pltpu.VMEM((2, 3, 2, 48, 512), BF16),
            pltpu.VMEM((2, 3, 64, 512), BF16),
            pltpu.VMEM((2, 3, 64, 512), BF16),
            pltpu.VMEM((2, 48, 512), BF16),
            pltpu.VMEM((2, 48, 512), BF16),
            pltpu.VMEM((2, 4, 64, 512), BF16),
            pltpu.VMEM((2, 4, 64, 512), BF16),
            pltpu.VMEM((2, 896, 128), F32),
            pltpu.VMEM((2, 16, 64, 128), BF16),
            pltpu.VMEM((2, 8, 64, 128), BF16),
            pltpu.VMEM((2, 8, 64, 128), BF16),
            pltpu.VMEM((2, 64, 128), F32),
            pltpu.VMEM((2, 64, 128), F32),
            pltpu.SemaphoreType.DMA((KINDS,)),
            pltpu.SemaphoreType.DMA((NAMES,)),
            pltpu.SemaphoreType.DMA((5,)),
        ],
        compiler_params=pltpu.CompilerParams(
            collective_id=0, has_side_effects=True, vmem_limit_bytes=65000 * 1024
        ),
    )(amplitudes, grid_factor, metric, virt_energy.reshape(7, 128), pair_energy)
    return jnp.transpose(out, (2, 0, 1))


def solution(mesh):
    in_specs = (P("blk", None, "grp"), P(("blk", "grp"), None), P("blk", "grp", None), P(), P())
    return jax.shard_map(
        local, mesh=mesh, in_specs=in_specs, out_specs=P("blk", None, "grp"), check_vma=False
    )
```

```python
import functools

import jax
import jax.numpy as jnp
from jax import lax
from jax.experimental import pallas as pl
from jax.experimental.pallas import tpu as pltpu
from jax.sharding import PartitionSpec as P

MESH = pl.DeviceIdType.MESH
F32 = jnp.float32
BF16 = jnp.bfloat16
NAMES, KINDS = 90, 15


class Links:
    def __init__(self, send, recv):
        self.send, self.recv, self.ids, self.kinds = send, recv, {}, {}

    def index(self, names, name, most):
        assert name in names or len(names) < most
        return names.setdefault(name, len(names))

    def copy(self, kind, name, src, dst, dev):
        return pltpu.make_async_remote_copy(
            src_ref=src, dst_ref=dst,
            send_sem=self.send.at[self.index(self.kinds, kind, KINDS)],
            recv_sem=self.recv.at[self.index(self.ids, name, NAMES)],
            device_id=dev, device_id_type=MESH,
        )

    def start(self, kind, name, src, dst, dev):
        self.copy(kind, name, src, dst, dev).start()

    def arrived(self, name, dst, dev):
        i = self.index(self.ids, name, NAMES)
        pltpu.make_async_remote_copy(
            src_ref=dst, dst_ref=dst, send_sem=self.send.at[0], recv_sem=self.recv.at[i],
            device_id=dev, device_id_type=MESH,
        ).wait_recv()

    def sent(self, kind, all_of_them, dev):
        pltpu.make_async_remote_copy(
            src_ref=all_of_them, dst_ref=all_of_them, send_sem=self.send.at[self.kinds[kind]],
            recv_sem=self.recv.at[0], device_id=dev, device_id_type=MESH,
        ).wait_send()


def kernel(
    amp_hbm, x_hbm, z_hbm, ve_hbm, pe_hbm, out_ref,
    amp, x_ref, ve, pe, tt_ref, own_amp, base,
    tall, xq, xqt, xp, xpt, zb, right, w, mp,
    e1s, e1r, e2s, e2r, e3s, e3r, eys, eyr, lad, fs, fy, fr, fins, finr,
    send, recv, local_sem,
):
    b, g = lax.axis_index("blk"), lax.axis_index("grp")
    core, yh, x = b % 2, (b // 2) % 2, b // 4
    yl, z = g // 8, g % 8
    m = x * 2 + yh
    net = Links(send, recv)

    def at(dx, dy, dc=0):
        yy = 1 - yh if dy else yh
        cc = 1 - core if dc else core
        return {"blk": ((x + dx + 4) % 4) * 4 + yy * 2 + cc, "grp": g}

    def up(dz, dyl=0, dc=0):
        return {
            "blk": b + 1 - 2 * core if dc else b,
            "grp": ((1 - yl) if dyl else yl) * 8 + (z + dz) % 8,
        }

    mate, xn, yp = at(0, 0, 1), at(1, 0), at(0, 1)
    zn, zv, yn = up(1), up(7), up(0, 1)
    around = [(2, 1), (3, 1), (1, 1), (2, 0), (3, 0), (1, 0)]

    def rows(dx, o, first=0, count=112):
        yy = 1 - yh if o else yh
        return pl.ds(pl.multiple_of((((x + dx + 4) % 4) * 2 + yy) * 112 + first, 16), count)

    def xqa(dx, dy):
        return xq.at[(1 - yh) if dy else yh, (x + dx + 4) % 4, core]

    def gi(dz, dyl):
        return ((1 - yl) if dyl else yl) * 8 + (z + dz + 8) % 8

    def xpa(dyl, dz):
        return xp.at[core, gi(dz, dyl)]

    def fetch(i, src, dst):
        c = pltpu.make_async_copy(src, dst, local_sem.at[i])
        c.start()
        return c

    acopy, xcopy = fetch(0, amp_hbm, amp), fetch(1, x_hbm, x_ref)
    barrier = pltpu.get_barrier_semaphore()
    near = [mate, yn] + [at(dx, 0) for dx in range(1, 4)]
    near += [yp] + [up(dz, 0, dc) for dz in range(1, 8) for dc in range(2)]
    with jax.named_scope("barrier"):
        for dev in near:
            pl.semaphore_signal(barrier, inc=1, device_id=dev, device_id_type=MESH)
        vcopy, pcopy = fetch(2, ve_hbm, ve.at[pl.ds(0, 7)]), fetch(3, pe_hbm, pe)
        zcopy = fetch(4, z_hbm.at[:, 0, :], zb.at[core])
        acopy.wait()
        eye = (
            lax.broadcasted_iota(jnp.int32, (56, 64), 0)
            == lax.broadcasted_iota(jnp.int32, (56, 64), 1)
        ).astype(BF16)
        for k in range(4):
            t = lax.dot_general(
                amp[:, k, :], eye, (((0,), (0,)), ((), ())), preferred_element_type=F32
            )
            own_amp[k] = t
            t = jnp.concatenate([t, jnp.zeros((8, 64), F32)], axis=0)
            tt_ref[k] = jnp.concatenate([t[:32], t[32:]], axis=1).astype(BF16)
        xcopy.wait()
        pl.semaphore_wait(barrier, len(near))

    far = (4, 3, 5, 2, 6, 1, 7)

    def t_send(k):
        net.start("t", ("t", k, 0), tt_ref.at[2 * (1 - core) + k], tall.at[k, core, g], mate)
        for dz in far:
            for dc in range(2):
                pair = 2 * ((1 - core) if dc else core) + k
                net.start("t", ("t", k, dz), tt_ref.at[pair], tall.at[k, core, g], up(dz, 0, dc))
        tall[k, core, g] = tt_ref[2 * core + k]

    def t_forward(k, dz):
        j = gi(-dz, 0)
        if dz:
            net.arrived(("t", k, dz), tall.at[k, :, j], up(8 - dz))
        else:
            net.arrived(("t", k, dz), tall.at[k, 1 - core, j], mate)
        net.start("ty", ("ty", k), tall.at[k, :, j], tall.at[k, :, j], yn)

    t_send(0)
    net.start("x", "xpy", x_ref, xpa(0, 0), yn)
    for dx, dy in ((0, 1), (1, 0), (3, 0), (2, 0)):
        net.start("x", ("xq", dx, dy), x_ref, xqa(0, 0), at(dx, dy))
    net.start("x", ("xqm", 0), x_ref, xqa(0, 0), mate)
    net.start("xp", ("xpn", 0, 1), x_ref, xpa(0, 0), zn)
    net.start("xp", ("xpv", 0, 1), x_ref, xpa(0, 0), zv)
    net.start("xpm", "xpm", x_ref, xpa(0, 0), mate)
    xq[yh, x, core] = x_ref[...]
    xp[core, g] = x_ref[...]

    def xq_forward(dx, dy):
        part = xqa(-dx, dy)
        net.arrived(("xq", dx, dy), part, at(4 - dx, 0 if dx else dy))
        if (dx, dy) == (0, 1):
            for to in (1, 3, 2):
                net.start("x", ("xq", to, 1), part, part, at(to, 0))
        net.start("x", ("xqm", dy), part, part, mate)

    lane = lax.broadcasted_iota(jnp.int32, (512, 128), 1)

    def gathered(k):
        net.arrived(("ty", k), tall.at[k, :, pl.ds(8 * (1 - yl), 8)], yn)
        one = tall[k, 0].reshape(512, 128).astype(F32)
        two = tall[k, 1].reshape(512, 128).astype(F32)
        top = jnp.where(lane < 64, one, pltpu.roll(two, 64, 1))
        low = jnp.where(lane < 64, pltpu.roll(one, 64, 1), two)
        t = jnp.concatenate(
            [v for j in range(16) for v in (top[32 * j : 32 * j + 32], low[32 * j : 32 * j + 24])],
            axis=0,
        )
        return t.astype(BF16)

    def first(k, t, half):
        rt = lax.dot_general(
            t, xq[half].reshape(256, 896), (((0,), (1,)), ((), ())), preferred_element_type=F32
        )
        cols = pl.ds(pl.multiple_of(half * 256, 256), 256)
        rt = jnp.concatenate([rt[:56], rt[64:120]], axis=0)
        right[k, rows(0, 0), cols] = rt.astype(BF16)
        return cols

    def r_send(k, cols):
        head, tail = right.at[k, rows(0, 0, 0, 64), cols], right.at[k, rows(0, 0, 64, 48), cols]
        net.start("r", ("ry", k), head, head, yp)
        for dx in (1, 3, 2):
            net.start("r", ("rx", k, dx), tail, tail, at(dx, 0))
        net.start("r", ("rw", k), tail, tail, yp)
        for dx in (1, 3, 2):
            net.start("r", ("rz", k), head, head, at(dx, 0))

    def xp_mate(dyl, dz):
        net.start("xpm", "xpm", xpa(dyl, dz), xpa(dyl, dz), mate)

    def xp_y():
        part = xpa(1, 0)
        net.arrived("xpy", part, yn)
        net.start("xp", ("xpn", 1, 1), part, part, zn)
        net.start("xp", ("xpv", 1, 1), part, part, zv)
        xp_mate(1, 0)

    def xp_step(s, dyl):
        if s < 4 or dyl == 0:
            part = xpa(dyl, -s)
            net.arrived(("xpn", dyl, s), part, zv)
            if s < 3 or (s == 3 and dyl == 0):
                net.start("xp", ("xpn", dyl, s + 1), part, part, zn)
            xp_mate(dyl, -s)
        if s < 4 or dyl == 1:
            part = xpa(dyl, s)
            net.arrived(("xpv", dyl, s), part, zn)
            if s < 3 or (s == 3 and dyl == 1):
                net.start("xp", ("xpv", dyl, s + 1), part, part, zv)
            xp_mate(dyl, s)

    def r_y(k):
        net.arrived(("ry", k), right.at[k, rows(0, 1, 0, 64)], yp)
        part = right.at[k, rows(0, 1, 0, 64)]
        for dx in (1, 3, 2):
            net.start("r2", ("rz", k), part, part, at(dx, 0))

    def r_x(k, *ways):
        for dx in ways:
            net.arrived(("rx", k, dx), right.at[k, rows(-dx, 0, 64, 48)], at(4 - dx, 0))
            part = right.at[k, rows(-dx, 0, 64, 48)]
            net.start("r2", ("rw", k), part, part, yp)

    def r_last(k):
        net.arrived(("rz", k), right.at[k, pl.ds(0, 384)], xn)
        net.arrived(("rw", k), right.at[k, pl.ds(0, 192)], yp)

    def weigh(k, c):
        p = jnp.dot(xp[c].reshape(512, 896), right[k], preferred_element_type=F32)
        w[512 * c : 512 * c + 512, :] = (zb[c] * p).astype(BF16)

    def mix(k, t):
        a = pl.ds(448 * t, 448)
        mp[k, a, :] = jnp.dot(xpt[a, :], w[...], preferred_element_type=F32)

    order = (2, 1, 3, 0)

    def e_start(k):
        for i, dx in enumerate(order):
            eys[k, i] = mp[k, rows(dx, 1, 48, 64), :].astype(BF16)
            net.start("ey", ("ey", k, dx), eys.at[k, i], eyr.at[k, i], yp)
            if dx:
                for o in range(2):
                    e1s[k, i, o] = mp[k, rows(dx, o, 0, 48), :].astype(BF16)
                net.start("e1", ("e1", k), e1s.at[k, i], e1r.at[k, i], at(dx, 0))

    def e_y(k, dx):
        i = order.index(dx)
        net.arrived(("ey", k, dx), eyr.at[k, i], yp)
        return mp[k, rows(dx, 0, 48, 64), :] + eyr[k, i].astype(F32)

    def e_two(k):
        for i, dx in enumerate(order[:3]):
            e2s[k, i] = e_y(k, dx).astype(BF16)
            net.start("e2", ("e2", k), e2s.at[k, i], e2r.at[k, i], at(dx, 0))

    def e_three(k):
        v = mp[k, rows(0, 1, 0, 48), :]
        net.arrived(("e1", k), e1r.at[k], xn)
        for i in range(3):
            v = v + e1r[k, i, 1].astype(F32)
        e3s[k] = v.astype(BF16)
        net.start("e3", ("e3", k), e3s.at[k], e3r.at[k], yp)

    def e_last(k):
        v = e_y(k, 0)
        net.arrived(("e2", k), e2r.at[k], xn)
        for i in range(3):
            v = v + e2r[k, i].astype(F32)
        u = mp[k, rows(0, 0, 0, 48), :]
        for i in range(3):
            u = u + e1r[k, i, 0].astype(F32)
        net.arrived(("e3", k), e3r.at[k], yp)
        return jnp.concatenate([u + e3r[k].astype(F32), v], axis=0)

    def ladder(k, v):
        gap = jnp.zeros((8, 512), F32)
        v = jnp.concatenate([v[:56], gap, v[56:], gap], axis=0).astype(BF16)
        lad[k] = lax.dot_general(
            xqt[...], v, (((1,), (1,)), ((), ())), preferred_element_type=F32
        )
        gap = jnp.zeros((8, 128), F32)
        for dz in range(8):
            j = gi(dz, 1)
            v = lad[k, pl.ds(pl.multiple_of(j * 56, 8), 56), :]
            fs[k, j] = jnp.concatenate([v, gap], axis=0).astype(BF16)
        for dz in far + (0,):
            net.start("fy", ("fy", k, dz), fs.at[k, gi(dz, 1)], fy.at[k, dz], yn)

    def fold(k):
        for dz in far + (0,):
            j = gi(dz, 0)
            net.arrived(("fy", k, dz), fy.at[k, dz], yn)
            v = lad[k, pl.ds(pl.multiple_of(j * 56, 8), 56), :] + fy[k, dz, 0:56].astype(F32)
            v = jnp.concatenate([v, jnp.zeros((8, 128), F32)], axis=0)
            if dz:
                fs[k, j] = v.astype(BF16)
                net.start("f", ("f", k), fs.at[k, j], fr.at[k, dz], up(dz))
            else:
                fins[k] = v

    def scoped(name, f, *args):
        with jax.named_scope(name):
            return f(*args)

    scoped("xp_y", xp_y)
    scoped("xq_y", xq_forward, 0, 1)
    with jax.named_scope("t0_xq"):
        t_forward(0, 0)
        for i, dz in enumerate(far[::-1]):
            t_forward(0, dz)
            if i < 3:
                xq_forward(*around[::-1][i])
    scoped("xp_step10", xp_step, 1, 0)
    scoped("xp_step11", xp_step, 1, 1)
    t_send(1)
    with jax.named_scope("first0a"):
        net.arrived(("xqm", 0), xq.at[yh, :, 1 - core], mate)
        t0 = gathered(0)
        r_send(0, first(0, t0, yh))
    with jax.named_scope("xq_far"):
        for dx, dy in around[2::-1]:
            xq_forward(dx, dy)
        net.arrived(("xqm", 1), xq.at[1 - yh, :, 1 - core], mate)
    with jax.named_scope("first0"):
        r_send(0, first(0, t0, 1 - yh))
    scoped("xp_step20", xp_step, 2, 0)
    scoped("xp_step21", xp_step, 2, 1)
    with jax.named_scope("xqt"):
        xqt[...] = jnp.transpose(xq[...].reshape(512, 896))
    with jax.named_scope("energies"):
        vcopy.wait()
        pcopy.wait()

        def run(start):
            r, off = start // 128, start % 128
            lane = lax.broadcasted_iota(jnp.int32, (8, 128), 1)
            one = jnp.broadcast_to(ve[pl.ds(r, 1), :], (8, 128))
            two = jnp.broadcast_to(ve[pl.ds(jnp.minimum(r + 1, 6), 1), :], (8, 128))
            shift = (128 - off) % 128
            return jnp.where(lane < 128 - off, pltpu.roll(one, shift, 1), pltpu.roll(two, shift, 1))

        first_e = run(b * 56)[0:1, :64]
        second_e = jnp.transpose(jnp.broadcast_to(run(g * 56)[0:1], (128, 128)))[:56, :64]
        both = second_e + first_e
        for k in range(4):
            base[k] = (both - pe[k]) * own_amp[k]
    with jax.named_scope("z_order"):
        zcopy.wait()

        def swap(i, carry):
            block = pl.ds(pl.multiple_of(64 * i, 64), 64)
            v = [zb[core, block, 128 * c : 128 * c + 128] for c in range(4)]
            u = [pltpu.roll(c, 64, 1) for c in v]
            low = lax.broadcasted_iota(jnp.int32, (64, 128), 1) < 64
            zb[core, block, 0:128] = jnp.where(low, v[0], u[1])
            zb[core, block, 128:256] = jnp.where(low, v[2], u[3])
            zb[core, block, 256:384] = jnp.where(low, u[0], v[1])
            zb[core, block, 384:512] = jnp.where(low, u[2], v[3])
            return carry

        lax.fori_loop(0, 8, swap, 0)
    net.start("z", "z", zb.at[core], zb.at[core], mate)
    with jax.named_scope("t1"):
        for dz in (0,) + far[::-1]:
            t_forward(1, dz)
    scoped("r_x01", r_x, 0, 1)
    scoped("xp_step30", xp_step, 3, 0)
    scoped("r_x03", r_x, 0, 3)
    scoped("xp_step31", xp_step, 3, 1)
    scoped("r_y0", r_y, 0)
    scoped("r_x02", r_x, 0, 2)
    with jax.named_scope("first1"):
        t1 = gathered(1)
        for half in range(2):
            first(1, t1, half)
        r_send(1, pl.ds(0, 512))
    scoped("xp_step40", xp_step, 4, 0)
    scoped("xp_step41", xp_step, 4, 1)
    with jax.named_scope("z_wait"):
        net.arrived("z", zb.at[1 - core], mate)
    with jax.named_scope("xpm_wait"):
        net.arrived("xpm", xp.at[1 - core], mate)
    with jax.named_scope("xpt"):
        for t in range(4):
            xpt[:, 256 * t : 256 * t + 256] = jnp.transpose(
                xp[t // 2, pl.ds(8 * (t % 2), 8)].reshape(256, 896)
            )
    scoped("r_last0", r_last, 0)
    scoped("weigh00", weigh, 0, 0)
    scoped("r_x11", r_x, 1, 1)
    scoped("r_x13", r_x, 1, 3)
    scoped("r_y1", r_y, 1)
    scoped("weigh01", weigh, 0, 1)
    scoped("r_x12", r_x, 1, 2)
    scoped("mix00", mix, 0, 0)
    scoped("mix01", mix, 0, 1)
    scoped("e_start0", e_start, 0)
    scoped("r_last1", r_last, 1)
    scoped("weigh10", weigh, 1, 0)
    scoped("weigh11", weigh, 1, 1)
    scoped("mix10", mix, 1, 0)
    scoped("mix11", mix, 1, 1)
    scoped("e_start1", e_start, 1)
    scoped("e_two0", e_two, 0)
    scoped("e_three0", e_three, 0)
    scoped("e_two1", e_two, 1)
    scoped("e_three1", e_three, 1)
    v0 = scoped("e_last0", e_last, 0)
    scoped("ladder0", ladder, 0, v0)
    v1 = scoped("e_last1", e_last, 1)
    scoped("ladder1", ladder, 1, v1)
    scoped("fold0", fold, 0)
    scoped("fold1", fold, 1)
    for k in range(2):
        total = fins[k]
        with jax.named_scope(f"f_wait{k}"):
            net.arrived(("f", k), fr.at[k, pl.ds(1, 7)], zn)
            for dz in far:
                total = total + fr[k, dz].astype(F32)
        fins[k] = total
        net.start("fin", ("fin", k), fins.at[k], finr.at[k], mate)
    def finish(pair, v):
        v = jnp.where(core == 0, v[:56, :64], v[:56, 64:]) + base[pair]
        out_ref[pair] = v[:, :56]

    for k in range(2):
        finish(2 * core + k, fins[k])
    with jax.named_scope("fin"):
        for k in range(2):
            net.arrived(("fin", k), finr.at[k], mate)
            finish(2 * (1 - core) + k, finr[k])
    with jax.named_scope("close"):
        for kind, whole in (
            ("t", tall.at[:, 0, pl.ds(0, 15)]), ("ty", tall.at[:, 0]), ("x", xq),
            ("xp", xp.at[0, pl.ds(0, 14)]), ("xpm", xp.at[0]), ("z", zb.at[0]),
            ("r", right.at[0]), ("r2", right.at[0, pl.ds(0, 672)]), ("ey", eys), ("e1", e1s),
            ("e2", e2s), ("e3", e3s), ("fy", fy), ("f", fr.at[:, pl.ds(0, 7)]), ("fin", fins),
        ):
            net.sent(kind, whole, mate)


def local(amplitudes, grid_factor, metric, virt_energy, pair_energy):
    rows, pairs, cols = amplitudes.shape
    hbm = pl.BlockSpec(memory_space=pltpu.HBM)
    out = pl.pallas_call(
        kernel,
        out_shape=pltpu.VMEM((pairs, cols, rows), F32),
        in_specs=[hbm] * 5,
        out_specs=pl.BlockSpec(memory_space=pltpu.VMEM),
        scratch_shapes=[
            pltpu.VMEM((56, 4, 56), BF16),
            pltpu.VMEM((32, 896), BF16),
            pltpu.VMEM((8, 128), F32),
            pltpu.SMEM((4,), F32),
            pltpu.VMEM((4, 32, 128), BF16),
            pltpu.VMEM((4, 56, 64), F32),
            pltpu.VMEM((4, 56, 64), F32),
            pltpu.VMEM((2, 2, 16, 32, 128), BF16),
            pltpu.VMEM((2, 4, 2, 32, 896), BF16),
            pltpu.VMEM((896, 512), BF16),
            pltpu.VMEM((2, 16, 32, 896), BF16),
            pltpu.VMEM((896, 1024), BF16),
            pltpu.VMEM((2, 512, 512), F32),
            pltpu.VMEM((2, 896, 512), BF16),
            pltpu.VMEM((1024, 512), BF16),
            pltpu.VMEM((2, 896, 512), F32),
            pltpu.VMEM((2, 3, 2, 48, 512), BF16),
            pltpu.VMEM((2, 3, 2, 48, 512), BF16),
            pltpu.VMEM((2, 3, 64, 512), BF16),
            pltpu.VMEM((2, 3, 64, 512), BF16),
            pltpu.VMEM((2, 48, 512), BF16),
            pltpu.VMEM((2, 48, 512), BF16),
            pltpu.VMEM((2, 4, 64, 512), BF16),
            pltpu.VMEM((2, 4, 64, 512), BF16),
            pltpu.VMEM((2, 896, 128), F32),
            pltpu.VMEM((2, 16, 64, 128), BF16),
            pltpu.VMEM((2, 8, 64, 128), BF16),
            pltpu.VMEM((2, 8, 64, 128), BF16),
            pltpu.VMEM((2, 64, 128), F32),
            pltpu.VMEM((2, 64, 128), F32),
            pltpu.SemaphoreType.DMA((KINDS,)),
            pltpu.SemaphoreType.DMA((NAMES,)),
            pltpu.SemaphoreType.DMA((5,)),
        ],
        compiler_params=pltpu.CompilerParams(
            collective_id=0, has_side_effects=True, vmem_limit_bytes=65000 * 1024
        ),
    )(amplitudes, grid_factor, metric, virt_energy.reshape(7, 128), pair_energy)
    return jnp.transpose(out, (2, 0, 1))


def solution(mesh):
    in_specs = (P("blk", None, "grp"), P(("blk", "grp"), None), P("blk", "grp", None), P(), P())
    return jax.shard_map(
        local, mesh=mesh, in_specs=in_specs, out_specs=P("blk", None, "grp"), check_vma=False
    )
```

```python
import functools

import jax
import jax.numpy as jnp
from jax import lax
from jax.experimental import pallas as pl
from jax.experimental.pallas import tpu as pltpu
from jax.sharding import PartitionSpec as P

MESH = pl.DeviceIdType.MESH
F32 = jnp.float32
BF16 = jnp.bfloat16
NAMES, KINDS = 90, 15


class Links:
    def __init__(self, send, recv):
        self.send, self.recv, self.ids, self.kinds = send, recv, {}, {}

    def index(self, names, name, most):
        assert name in names or len(names) < most
        return names.setdefault(name, len(names))

    def copy(self, kind, name, src, dst, dev):
        return pltpu.make_async_remote_copy(
            src_ref=src, dst_ref=dst,
            send_sem=self.send.at[self.index(self.kinds, kind, KINDS)],
            recv_sem=self.recv.at[self.index(self.ids, name, NAMES)],
            device_id=dev, device_id_type=MESH,
        )

    def start(self, kind, name, src, dst, dev):
        self.copy(kind, name, src, dst, dev).start()

    def arrived(self, name, dst, dev):
        i = self.index(self.ids, name, NAMES)
        pltpu.make_async_remote_copy(
            src_ref=dst, dst_ref=dst, send_sem=self.send.at[0], recv_sem=self.recv.at[i],
            device_id=dev, device_id_type=MESH,
        ).wait_recv()

    def sent(self, kind, all_of_them, dev):
        pltpu.make_async_remote_copy(
            src_ref=all_of_them, dst_ref=all_of_them, send_sem=self.send.at[self.kinds[kind]],
            recv_sem=self.recv.at[0], device_id=dev, device_id_type=MESH,
        ).wait_send()


def kernel(
    amp_hbm, x_hbm, z_hbm, ve_hbm, pe_hbm, out_ref,
    amp, x_ref, ve, pe, tt_ref, own_amp, base,
    tall, xq, xqt, xp, xpt, zb, right, w, mp,
    e1s, e1r, e2s, e2r, e3s, e3r, eys, eyr, lad, fs, fy, fr, fins, finr,
    send, recv, local_sem,
):
    b, g = lax.axis_index("blk"), lax.axis_index("grp")
    core, yh, x = b % 2, (b // 2) % 2, b // 4
    yl, z = g // 8, g % 8
    m = x * 2 + yh
    net = Links(send, recv)

    def at(dx, dy, dc=0):
        yy = 1 - yh if dy else yh
        cc = 1 - core if dc else core
        return {"blk": ((x + dx + 4) % 4) * 4 + yy * 2 + cc, "grp": g}

    def up(dz, dyl=0, dc=0):
        return {
            "blk": b + 1 - 2 * core if dc else b,
            "grp": ((1 - yl) if dyl else yl) * 8 + (z + dz) % 8,
        }

    mate, xn, yp = at(0, 0, 1), at(1, 0), at(0, 1)
    zn, zv, yn = up(1), up(7), up(0, 1)
    around = [(2, 1), (3, 1), (1, 1), (2, 0), (3, 0), (1, 0)]

    def rows(dx, o, first=0, count=112):
        yy = 1 - yh if o else yh
        return pl.ds(pl.multiple_of((((x + dx + 4) % 4) * 2 + yy) * 112 + first, 16), count)

    def xqa(dx, dy):
        return xq.at[(1 - yh) if dy else yh, (x + dx + 4) % 4, core]

    def gi(dz, dyl):
        return ((1 - yl) if dyl else yl) * 8 + (z + dz + 8) % 8

    def xpa(dyl, dz):
        return xp.at[core, gi(dz, dyl)]

    def fetch(i, src, dst):
        c = pltpu.make_async_copy(src, dst, local_sem.at[i])
        c.start()
        return c

    acopy, xcopy = fetch(0, amp_hbm, amp), fetch(1, x_hbm, x_ref)
    barrier = pltpu.get_barrier_semaphore()
    near = [mate, yn] + [at(dx, 0) for dx in range(1, 4)]
    near += [yp] + [up(dz, 0, dc) for dz in range(1, 8) for dc in range(2)]
    with jax.named_scope("barrier"):
        for dev in near:
            pl.semaphore_signal(barrier, inc=1, device_id=dev, device_id_type=MESH)
        vcopy, pcopy = fetch(2, ve_hbm, ve.at[pl.ds(0, 7)]), fetch(3, pe_hbm, pe)
        zcopy = fetch(4, z_hbm.at[:, 0, :], zb.at[core])
        acopy.wait()
        eye = (
            lax.broadcasted_iota(jnp.int32, (56, 64), 0)
            == lax.broadcasted_iota(jnp.int32, (56, 64), 1)
        ).astype(BF16)
        for k in range(4):
            t = lax.dot_general(
                amp[:, k, :], eye, (((0,), (0,)), ((), ())), preferred_element_type=F32
            )
            own_amp[k] = t
            t = jnp.concatenate([t, jnp.zeros((8, 64), F32)], axis=0)
            tt_ref[k] = jnp.concatenate([t[:32], t[32:]], axis=1).astype(BF16)
        xcopy.wait()
        pl.semaphore_wait(barrier, len(near))

    far, mixed = (4, 3, 5, 2, 6, 1, 7), (4, 1, 7, 3, 5, 2, 6)

    def t_send(k):
        net.start("t", ("t", k, 0), tt_ref.at[2 * (1 - core) + k], tall.at[k, core, g], mate)
        for dz in mixed:
            for dc in range(2):
                pair = 2 * ((1 - core) if dc else core) + k
                net.start("t", ("t", k, dz), tt_ref.at[pair], tall.at[k, core, g], up(dz, 0, dc))
        tall[k, core, g] = tt_ref[2 * core + k]

    def t_forward(k, dz):
        j = gi(-dz, 0)
        if dz:
            net.arrived(("t", k, dz), tall.at[k, :, j], up(8 - dz))
        else:
            net.arrived(("t", k, dz), tall.at[k, 1 - core, j], mate)
        net.start("ty", ("ty", k), tall.at[k, :, j], tall.at[k, :, j], yn)

    t_send(0)
    net.start("x", "xpy", x_ref, xpa(0, 0), yn)
    for dx, dy in ((0, 1), (1, 0), (3, 0), (2, 0)):
        net.start("x", ("xq", dx, dy), x_ref, xqa(0, 0), at(dx, dy))
    net.start("x", ("xqm", 0), x_ref, xqa(0, 0), mate)
    net.start("xp", ("xpn", 0, 1), x_ref, xpa(0, 0), zn)
    net.start("xp", ("xpv", 0, 1), x_ref, xpa(0, 0), zv)
    net.start("xpm", "xpm", x_ref, xpa(0, 0), mate)
    xq[yh, x, core] = x_ref[...]
    xp[core, g] = x_ref[...]

    def xq_forward(dx, dy):
        part = xqa(-dx, dy)
        net.arrived(("xq", dx, dy), part, at(4 - dx, 0 if dx else dy))
        if (dx, dy) == (0, 1):
            for to in (1, 3, 2):
                net.start("x", ("xq", to, 1), part, part, at(to, 0))
        net.start("x", ("xqm", dy), part, part, mate)

    lane = lax.broadcasted_iota(jnp.int32, (512, 128), 1)

    def gathered(k):
        net.arrived(("ty", k), tall.at[k, :, pl.ds(8 * (1 - yl), 8)], yn)
        one = tall[k, 0].reshape(512, 128).astype(F32)
        two = tall[k, 1].reshape(512, 128).astype(F32)
        top = jnp.where(lane < 64, one, pltpu.roll(two, 64, 1))
        low = jnp.where(lane < 64, pltpu.roll(one, 64, 1), two)
        t = jnp.concatenate(
            [v for j in range(16) for v in (top[32 * j : 32 * j + 32], low[32 * j : 32 * j + 24])],
            axis=0,
        )
        return t.astype(BF16)

    def first(k, t, half):
        rt = lax.dot_general(
            t, xq[half].reshape(256, 896), (((0,), (1,)), ((), ())), preferred_element_type=F32
        )
        cols = pl.ds(pl.multiple_of(half * 256, 256), 256)
        rt = jnp.concatenate([rt[:56], rt[64:120]], axis=0)
        right[k, rows(0, 0), cols] = rt.astype(BF16)
        return cols

    def r_send(k, cols):
        head, tail = right.at[k, rows(0, 0, 0, 64), cols], right.at[k, rows(0, 0, 64, 48), cols]
        net.start("r", ("ry", k), head, head, yp)
        for dx in (1, 3, 2):
            net.start("r", ("rx", k, dx), tail, tail, at(dx, 0))
        net.start("r", ("rw", k), tail, tail, yp)
        for dx in (1, 3, 2):
            net.start("r", ("rz", k), head, head, at(dx, 0))

    def xp_mate(dyl, dz):
        net.start("xpm", "xpm", xpa(dyl, dz), xpa(dyl, dz), mate)

    def xp_y():
        part = xpa(1, 0)
        net.arrived("xpy", part, yn)
        net.start("xp", ("xpn", 1, 1), part, part, zn)
        net.start("xp", ("xpv", 1, 1), part, part, zv)
        xp_mate(1, 0)

    def xp_step(s, dyl):
        if s < 4 or dyl == 0:
            part = xpa(dyl, -s)
            net.arrived(("xpn", dyl, s), part, zv)
            if s < 3 or (s == 3 and dyl == 0):
                net.start("xp", ("xpn", dyl, s + 1), part, part, zn)
            xp_mate(dyl, -s)
        if s < 4 or dyl == 1:
            part = xpa(dyl, s)
            net.arrived(("xpv", dyl, s), part, zn)
            if s < 3 or (s == 3 and dyl == 1):
                net.start("xp", ("xpv", dyl, s + 1), part, part, zv)
            xp_mate(dyl, s)

    def r_y(k):
        net.arrived(("ry", k), right.at[k, rows(0, 1, 0, 64)], yp)
        part = right.at[k, rows(0, 1, 0, 64)]
        for dx in (1, 3, 2):
            net.start("r2", ("rz", k), part, part, at(dx, 0))

    def r_x(k, *ways):
        for dx in ways:
            net.arrived(("rx", k, dx), right.at[k, rows(-dx, 0, 64, 48)], at(4 - dx, 0))
            part = right.at[k, rows(-dx, 0, 64, 48)]
            net.start("r2", ("rw", k), part, part, yp)

    def r_last(k):
        net.arrived(("rz", k), right.at[k, pl.ds(0, 384)], xn)
        net.arrived(("rw", k), right.at[k, pl.ds(0, 192)], yp)

    def weigh(k, c):
        p = jnp.dot(xp[c].reshape(512, 896), right[k], preferred_element_type=F32)
        w[512 * c : 512 * c + 512, :] = (zb[c] * p).astype(BF16)

    def mix(k, t):
        a = pl.ds(448 * t, 448)
        mp[k, a, :] = jnp.dot(xpt[a, :], w[...], preferred_element_type=F32)

    order = (2, 1, 3, 0)

    def e_start(k):
        for i, dx in enumerate(order):
            eys[k, i] = mp[k, rows(dx, 1, 48, 64), :].astype(BF16)
            net.start("ey", ("ey", k, dx), eys.at[k, i], eyr.at[k, i], yp)
            if dx:
                for o in range(2):
                    e1s[k, i, o] = mp[k, rows(dx, o, 0, 48), :].astype(BF16)
                net.start("e1", ("e1", k), e1s.at[k, i], e1r.at[k, i], at(dx, 0))

    def e_y(k, dx):
        i = order.index(dx)
        net.arrived(("ey", k, dx), eyr.at[k, i], yp)
        return mp[k, rows(dx, 0, 48, 64), :] + eyr[k, i].astype(F32)

    def e_two(k):
        for i, dx in enumerate(order[:3]):
            e2s[k, i] = e_y(k, dx).astype(BF16)
            net.start("e2", ("e2", k), e2s.at[k, i], e2r.at[k, i], at(dx, 0))

    def e_three(k):
        v = mp[k, rows(0, 1, 0, 48), :]
        net.arrived(("e1", k), e1r.at[k], xn)
        for i in range(3):
            v = v + e1r[k, i, 1].astype(F32)
        e3s[k] = v.astype(BF16)
        net.start("e3", ("e3", k), e3s.at[k], e3r.at[k], yp)

    def e_last(k):
        v = e_y(k, 0)
        net.arrived(("e2", k), e2r.at[k], xn)
        for i in range(3):
            v = v + e2r[k, i].astype(F32)
        u = mp[k, rows(0, 0, 0, 48), :]
        for i in range(3):
            u = u + e1r[k, i, 0].astype(F32)
        net.arrived(("e3", k), e3r.at[k], yp)
        return jnp.concatenate([u + e3r[k].astype(F32), v], axis=0)

    def ladder(k, v):
        gap = jnp.zeros((8, 512), F32)
        v = jnp.concatenate([v[:56], gap, v[56:], gap], axis=0).astype(BF16)
        for column in (1 - yl, yl):
            part = pl.ds(pl.multiple_of(column * 448, 64), 448)
            lad[k, part] = lax.dot_general(
                xqt[part, :], v, (((1,), (1,)), ((), ())), preferred_element_type=F32
            )
            if column is not yl:
                for dz in far + (0,):
                    j = gi(dz, 1)
                    u = lad[k, pl.ds(pl.multiple_of(j * 56, 8), 56), :]
                    fs[k, j] = u.astype(BF16)
                    net.start("fy", ("fy", k, dz), fs.at[k, j], fy.at[k, dz], yn)

    def fold(k):
        for dz in far + (0,):
            j = gi(dz, 0)
            net.arrived(("fy", k, dz), fy.at[k, dz], yn)
            v = lad[k, pl.ds(pl.multiple_of(j * 56, 8), 56), :] + fy[k, dz].astype(F32)
            if dz:
                fs[k, j] = v.astype(BF16)
                net.start("f", ("f", k), fs.at[k, j], fr.at[k, dz], up(dz))
            else:
                fins[k] = v

    def scoped(name, f, *args):
        with jax.named_scope(name):
            return f(*args)

    scoped("t00", t_forward, 0, 0)
    scoped("xp_y", xp_y)
    scoped("t01", t_forward, 0, 1)
    scoped("t07", t_forward, 0, 7)
    scoped("xq_y", xq_forward, 0, 1)
    with jax.named_scope("t0_xq"):
        for i, dz in enumerate((4, 3, 5, 2, 6)):
            t_forward(0, dz)
            if i < 3:
                xq_forward(*around[::-1][i])
    t_send(1)
    scoped("xp_step10", xp_step, 1, 0)
    scoped("xp_step11", xp_step, 1, 1)
    with jax.named_scope("first0a"):
        net.arrived(("xqm", 0), xq.at[yh, :, 1 - core], mate)
        t0 = gathered(0)
        r_send(0, first(0, t0, yh))
    with jax.named_scope("xq_far"):
        for dx, dy in around[2::-1]:
            xq_forward(dx, dy)
        net.arrived(("xqm", 1), xq.at[1 - yh, :, 1 - core], mate)
    with jax.named_scope("first0"):
        r_send(0, first(0, t0, 1 - yh))
    scoped("xp_step20", xp_step, 2, 0)
    scoped("xp_step21", xp_step, 2, 1)
    with jax.named_scope("xqt"):
        xqt[...] = jnp.transpose(xq[...].reshape(512, 896))
    with jax.named_scope("energies"):
        vcopy.wait()
        pcopy.wait()

        def run(start):
            r, off = start // 128, start % 128
            lane = lax.broadcasted_iota(jnp.int32, (8, 128), 1)
            one = jnp.broadcast_to(ve[pl.ds(r, 1), :], (8, 128))
            two = jnp.broadcast_to(ve[pl.ds(jnp.minimum(r + 1, 6), 1), :], (8, 128))
            shift = (128 - off) % 128
            return jnp.where(lane < 128 - off, pltpu.roll(one, shift, 1), pltpu.roll(two, shift, 1))

        first_e = run(b * 56)[0:1, :64]
        second_e = jnp.transpose(jnp.broadcast_to(run(g * 56)[0:1], (128, 128)))[:56, :64]
        both = second_e + first_e
        for k in range(4):
            base[k] = (both - pe[k]) * own_amp[k]
    with jax.named_scope("t1"):
        for dz in (0, 1, 7, 4, 3, 5, 2, 6):
            t_forward(1, dz)
    with jax.named_scope("z_order"):
        zcopy.wait()

        def swap(i, carry):
            block = pl.ds(pl.multiple_of(64 * i, 64), 64)
            v = [zb[core, block, 128 * c : 128 * c + 128] for c in range(4)]
            u = [pltpu.roll(c, 64, 1) for c in v]
            low = lax.broadcasted_iota(jnp.int32, (64, 128), 1) < 64
            zb[core, block, 0:128] = jnp.where(low, v[0], u[1])
            zb[core, block, 128:256] = jnp.where(low, v[2], u[3])
            zb[core, block, 256:384] = jnp.where(low, u[0], v[1])
            zb[core, block, 384:512] = jnp.where(low, u[2], v[3])
            return carry

        lax.fori_loop(0, 8, swap, 0)
    net.start("z", "z", zb.at[core], zb.at[core], mate)
    scoped("r_x01", r_x, 0, 1)
    scoped("xp_step30", xp_step, 3, 0)
    scoped("r_x03", r_x, 0, 3)
    scoped("xp_step31", xp_step, 3, 1)
    scoped("r_y0", r_y, 0)
    scoped("r_x02", r_x, 0, 2)
    with jax.named_scope("first1"):
        t1 = gathered(1)
        for half in range(2):
            first(1, t1, half)
        r_send(1, pl.ds(0, 512))
    scoped("xp_step40", xp_step, 4, 0)
    scoped("xp_step41", xp_step, 4, 1)
    with jax.named_scope("z_wait"):
        net.arrived("z", zb.at[1 - core], mate)
    with jax.named_scope("xpm_wait"):
        net.arrived("xpm", xp.at[1 - core], mate)
    with jax.named_scope("xpt"):
        for t in range(4):
            xpt[:, 256 * t : 256 * t + 256] = jnp.transpose(
                xp[t // 2, pl.ds(8 * (t % 2), 8)].reshape(256, 896)
            )
    scoped("r_last0", r_last, 0)
    scoped("weigh00", weigh, 0, 0)
    scoped("r_x11", r_x, 1, 1)
    scoped("r_x13", r_x, 1, 3)
    scoped("r_y1", r_y, 1)
    scoped("weigh01", weigh, 0, 1)
    scoped("r_x12", r_x, 1, 2)
    scoped("mix00", mix, 0, 0)
    scoped("mix01", mix, 0, 1)
    scoped("e_start0", e_start, 0)
    scoped("r_last1", r_last, 1)
    scoped("weigh10", weigh, 1, 0)
    scoped("weigh11", weigh, 1, 1)
    scoped("mix10", mix, 1, 0)
    scoped("mix11", mix, 1, 1)
    scoped("e_start1", e_start, 1)
    scoped("e_two0", e_two, 0)
    scoped("e_three0", e_three, 0)
    scoped("e_two1", e_two, 1)
    scoped("e_three1", e_three, 1)
    v0 = scoped("e_last0", e_last, 0)
    scoped("ladder0", ladder, 0, v0)
    v1 = scoped("e_last1", e_last, 1)
    scoped("ladder1", ladder, 1, v1)
    scoped("fold0", fold, 0)
    scoped("fold1", fold, 1)
    for k in range(2):
        total = fins[k]
        with jax.named_scope(f"f_wait{k}"):
            net.arrived(("f", k), fr.at[k, pl.ds(1, 7)], zn)
            for dz in far:
                total = total + fr[k, dz].astype(F32)
        fins[k] = total
        net.start("fin", ("fin", k), fins.at[k], finr.at[k], mate)
    def finish(pair, v):
        v = jnp.where(core == 0, v[:, :64], v[:, 64:]) + base[pair]
        out_ref[pair] = v[:, :56]

    for k in range(2):
        finish(2 * core + k, fins[k])
    with jax.named_scope("fin"):
        for k in range(2):
            net.arrived(("fin", k), finr.at[k], mate)
            finish(2 * (1 - core) + k, finr[k])
    with jax.named_scope("close"):
        for kind, whole in (
            ("t", tall.at[:, 0, pl.ds(0, 15)]), ("ty", tall.at[:, 0]), ("x", xq),
            ("xp", xp.at[0, pl.ds(0, 14)]), ("xpm", xp.at[0]), ("z", zb.at[0]),
            ("r", right.at[0]), ("r2", right.at[0, pl.ds(0, 672)]), ("ey", eys), ("e1", e1s),
            ("e2", e2s), ("e3", e3s), ("fy", fy), ("f", fr.at[:, pl.ds(0, 7)]), ("fin", fins),
        ):
            net.sent(kind, whole, mate)


def local(amplitudes, grid_factor, metric, virt_energy, pair_energy):
    rows, pairs, cols = amplitudes.shape
    hbm = pl.BlockSpec(memory_space=pltpu.HBM)
    out = pl.pallas_call(
        kernel,
        out_shape=pltpu.VMEM((pairs, cols, rows), F32),
        in_specs=[hbm] * 5,
        out_specs=pl.BlockSpec(memory_space=pltpu.VMEM),
        scratch_shapes=[
            pltpu.VMEM((56, 4, 56), BF16),
            pltpu.VMEM((32, 896), BF16),
            pltpu.VMEM((8, 128), F32),
            pltpu.SMEM((4,), F32),
            pltpu.VMEM((4, 32, 128), BF16),
            pltpu.VMEM((4, 56, 64), F32),
            pltpu.VMEM((4, 56, 64), F32),
            pltpu.VMEM((2, 2, 16, 32, 128), BF16),
            pltpu.VMEM((2, 4, 2, 32, 896), BF16),
            pltpu.VMEM((896, 512), BF16),
            pltpu.VMEM((2, 16, 32, 896), BF16),
            pltpu.VMEM((896, 1024), BF16),
            pltpu.VMEM((2, 512, 512), F32),
            pltpu.VMEM((2, 896, 512), BF16),
            pltpu.VMEM((1024, 512), BF16),
            pltpu.VMEM((2, 896, 512), F32),
            pltpu.VMEM((2, 3, 2, 48, 512), BF16),
            pltpu.VMEM((2, 3, 2, 48, 512), BF16),
            pltpu.VMEM((2, 3, 64, 512), BF16),
            pltpu.VMEM((2, 3, 64, 512), BF16),
            pltpu.VMEM((2, 48, 512), BF16),
            pltpu.VMEM((2, 48, 512), BF16),
            pltpu.VMEM((2, 4, 64, 512), BF16),
            pltpu.VMEM((2, 4, 64, 512), BF16),
            pltpu.VMEM((2, 896, 128), F32),
            pltpu.VMEM((2, 16, 56, 128), BF16),
            pltpu.VMEM((2, 8, 56, 128), BF16),
            pltpu.VMEM((2, 8, 56, 128), BF16),
            pltpu.VMEM((2, 56, 128), F32),
            pltpu.VMEM((2, 56, 128), F32),
            pltpu.SemaphoreType.DMA((KINDS,)),
            pltpu.SemaphoreType.DMA((NAMES,)),
            pltpu.SemaphoreType.DMA((5,)),
        ],
        compiler_params=pltpu.CompilerParams(
            collective_id=0, has_side_effects=True, vmem_limit_bytes=65000 * 1024
        ),
    )(amplitudes, grid_factor, metric, virt_energy.reshape(7, 128), pair_energy)
    return jnp.transpose(out, (2, 0, 1))


def solution(mesh):
    in_specs = (P("blk", None, "grp"), P(("blk", "grp"), None), P("blk", "grp", None), P(), P())
    return jax.shard_map(
        local, mesh=mesh, in_specs=in_specs, out_specs=P("blk", None, "grp"), check_vma=False
    )
```

```python
import functools

import jax
import jax.numpy as jnp
from jax import lax
from jax.experimental import pallas as pl
from jax.experimental.pallas import tpu as pltpu
from jax.sharding import PartitionSpec as P

MESH = pl.DeviceIdType.MESH
F32 = jnp.float32
BF16 = jnp.bfloat16
NAMES, KINDS = 90, 15


class Links:
    def __init__(self, send, recv):
        self.send, self.recv, self.ids, self.kinds = send, recv, {}, {}

    def index(self, names, name, most):
        assert name in names or len(names) < most
        return names.setdefault(name, len(names))

    def copy(self, kind, name, src, dst, dev):
        return pltpu.make_async_remote_copy(
            src_ref=src, dst_ref=dst,
            send_sem=self.send.at[self.index(self.kinds, kind, KINDS)],
            recv_sem=self.recv.at[self.index(self.ids, name, NAMES)],
            device_id=dev, device_id_type=MESH,
        )

    def start(self, kind, name, src, dst, dev):
        self.copy(kind, name, src, dst, dev).start()

    def arrived(self, name, dst, dev):
        i = self.index(self.ids, name, NAMES)
        pltpu.make_async_remote_copy(
            src_ref=dst, dst_ref=dst, send_sem=self.send.at[0], recv_sem=self.recv.at[i],
            device_id=dev, device_id_type=MESH,
        ).wait_recv()

    def sent(self, kind, all_of_them, dev):
        pltpu.make_async_remote_copy(
            src_ref=all_of_them, dst_ref=all_of_them, send_sem=self.send.at[self.kinds[kind]],
            recv_sem=self.recv.at[0], device_id=dev, device_id_type=MESH,
        ).wait_send()


def kernel(
    amp_hbm, x_hbm, z_hbm, ve_hbm, pe_hbm, out_ref,
    amp, x_ref, ve, pe, tt_ref, own_amp, base,
    tall, xq, xqt, xp, xpt, zb, right, w, mp,
    e1s, e1r, e2s, e2r, e3s, e3r, eys, eyr, lad, fs, fy, fr, fins, finr,
    send, recv, local_sem,
):
    b, g = lax.axis_index("blk"), lax.axis_index("grp")
    core, yh, x = b % 2, (b // 2) % 2, b // 4
    yl, z = g // 8, g % 8
    m = x * 2 + yh
    net = Links(send, recv)

    def at(dx, dy, dc=0):
        yy = 1 - yh if dy else yh
        cc = 1 - core if dc else core
        return {"blk": ((x + dx + 4) % 4) * 4 + yy * 2 + cc, "grp": g}

    def up(dz, dyl=0, dc=0):
        return {
            "blk": b + 1 - 2 * core if dc else b,
            "grp": ((1 - yl) if dyl else yl) * 8 + (z + dz) % 8,
        }

    mate, xn, yp = at(0, 0, 1), at(1, 0), at(0, 1)
    zn, zv, yn = up(1), up(7), up(0, 1)
    around = [(2, 1), (3, 1), (1, 1), (2, 0), (3, 0), (1, 0)]

    def rows(dx, o, first=0, count=112):
        yy = 1 - yh if o else yh
        return pl.ds(pl.multiple_of((((x + dx + 4) % 4) * 2 + yy) * 112 + first, 16), count)

    def xqa(dx, dy):
        return xq.at[(1 - yh) if dy else yh, (x + dx + 4) % 4, core]

    def gi(dz, dyl):
        return ((1 - yl) if dyl else yl) * 8 + (z + dz + 8) % 8

    def xpa(dyl, dz):
        return xp.at[core, gi(dz, dyl)]

    def fetch(i, src, dst):
        c = pltpu.make_async_copy(src, dst, local_sem.at[i])
        c.start()
        return c

    acopy, xcopy = fetch(0, amp_hbm, amp), fetch(1, x_hbm, x_ref)
    barrier = pltpu.get_barrier_semaphore()
    near = [mate, yn] + [at(dx, 0) for dx in range(1, 4)]
    near += [yp] + [up(dz, 0, dc) for dz in range(1, 8) for dc in range(2)]
    with jax.named_scope("barrier"):
        for dev in near:
            pl.semaphore_signal(barrier, inc=1, device_id=dev, device_id_type=MESH)
        vcopy, pcopy = fetch(2, ve_hbm, ve.at[pl.ds(0, 7)]), fetch(3, pe_hbm, pe)
        zcopy = fetch(4, z_hbm.at[:, 0, :], zb.at[core])
        xcopy.wait()
        pl.semaphore_wait(barrier, len(near))

    far, mixed = (4, 3, 5, 2, 6, 1, 7), (4, 1, 7, 3, 5, 2, 6)

    def t_send(k):
        net.start("t", ("t", k, 0), tt_ref.at[2 * (1 - core) + k], tall.at[k, core, g], mate)
        for dz in mixed:
            for dc in range(2):
                pair = 2 * ((1 - core) if dc else core) + k
                net.start("t", ("t", k, dz), tt_ref.at[pair], tall.at[k, core, g], up(dz, 0, dc))
        tall[k, core, g] = tt_ref[2 * core + k]

    def t_forward(k, dz):
        j = gi(-dz, 0)
        if dz:
            net.arrived(("t", k, dz), tall.at[k, :, j], up(8 - dz))
        else:
            net.arrived(("t", k, dz), tall.at[k, 1 - core, j], mate)
        net.start("ty", ("ty", k), tall.at[k, :, j], tall.at[k, :, j], yn)

    net.start("x", "xpy", x_ref, xpa(0, 0), yn)
    for dx, dy in ((0, 1), (1, 0), (3, 0), (2, 0)):
        net.start("x", ("xq", dx, dy), x_ref, xqa(0, 0), at(dx, dy))
    net.start("x", ("xqm", 0), x_ref, xqa(0, 0), mate)
    acopy.wait()
    eye = (
        lax.broadcasted_iota(jnp.int32, (56, 64), 0)
        == lax.broadcasted_iota(jnp.int32, (56, 64), 1)
    ).astype(BF16)
    for k in range(4):
        t = lax.dot_general(
            amp[:, k, :], eye, (((0,), (0,)), ((), ())), preferred_element_type=F32
        )
        own_amp[k] = t
        t = jnp.concatenate([t, jnp.zeros((8, 64), F32)], axis=0)
        tt_ref[k] = jnp.concatenate([t[:32], t[32:]], axis=1).astype(BF16)
    t_send(0)
    net.start("xp", ("xpn", 0, 1), x_ref, xpa(0, 0), zn)
    net.start("xp", ("xpv", 0, 1), x_ref, xpa(0, 0), zv)
    net.start("xpm", "xpm", x_ref, xpa(0, 0), mate)
    xq[yh, x, core] = x_ref[...]
    xp[core, g] = x_ref[...]

    def xq_forward(dx, dy):
        part = xqa(-dx, dy)
        net.arrived(("xq", dx, dy), part, at(4 - dx, 0 if dx else dy))
        if (dx, dy) == (0, 1):
            for to in (1, 3, 2):
                net.start("x", ("xq", to, 1), part, part, at(to, 0))
        net.start("x", ("xqm", dy), part, part, mate)

    lane = lax.broadcasted_iota(jnp.int32, (512, 128), 1)

    def gathered(k):
        net.arrived(("ty", k), tall.at[k, :, pl.ds(8 * (1 - yl), 8)], yn)
        one = tall[k, 0].reshape(512, 128).astype(F32)
        two = tall[k, 1].reshape(512, 128).astype(F32)
        top = jnp.where(lane < 64, one, pltpu.roll(two, 64, 1))
        low = jnp.where(lane < 64, pltpu.roll(one, 64, 1), two)
        t = jnp.concatenate(
            [v for j in range(16) for v in (top[32 * j : 32 * j + 32], low[32 * j : 32 * j + 24])],
            axis=0,
        )
        return t.astype(BF16)

    def first(k, t, half):
        rt = lax.dot_general(
            t, xq[half].reshape(256, 896), (((0,), (1,)), ((), ())), preferred_element_type=F32
        )
        cols = pl.ds(pl.multiple_of(half * 256, 256), 256)
        rt = jnp.concatenate([rt[:56], rt[64:120]], axis=0)
        right[k, rows(0, 0), cols] = rt.astype(BF16)
        return cols

    def r_send(k, cols):
        head, tail = right.at[k, rows(0, 0, 0, 64), cols], right.at[k, rows(0, 0, 64, 48), cols]
        net.start("r", ("ry", k), head, head, yp)
        for dx in (1, 3, 2):
            net.start("r", ("rx", k, dx), tail, tail, at(dx, 0))
        net.start("r", ("rw", k), tail, tail, yp)
        for dx in (1, 3, 2):
            net.start("r", ("rz", k), head, head, at(dx, 0))

    def xp_mate(dyl, dz):
        net.start("xpm", "xpm", xpa(dyl, dz), xpa(dyl, dz), mate)

    def xp_y():
        part = xpa(1, 0)
        net.arrived("xpy", part, yn)
        net.start("xp", ("xpn", 1, 1), part, part, zn)
        net.start("xp", ("xpv", 1, 1), part, part, zv)
        xp_mate(1, 0)

    def xp_step(s, dyl):
        if s < 4 or dyl == 0:
            part = xpa(dyl, -s)
            net.arrived(("xpn", dyl, s), part, zv)
            if s < 3 or (s == 3 and dyl == 0):
                net.start("xp", ("xpn", dyl, s + 1), part, part, zn)
            xp_mate(dyl, -s)
        if s < 4 or dyl == 1:
            part = xpa(dyl, s)
            net.arrived(("xpv", dyl, s), part, zn)
            if s < 3 or (s == 3 and dyl == 1):
                net.start("xp", ("xpv", dyl, s + 1), part, part, zv)
            xp_mate(dyl, s)

    def r_y(k):
        net.arrived(("ry", k), right.at[k, rows(0, 1, 0, 64)], yp)
        part = right.at[k, rows(0, 1, 0, 64)]
        for dx in (1, 3, 2):
            net.start("r2", ("rz", k), part, part, at(dx, 0))

    def r_x(k, *ways):
        for dx in ways:
            net.arrived(("rx", k, dx), right.at[k, rows(-dx, 0, 64, 48)], at(4 - dx, 0))
            part = right.at[k, rows(-dx, 0, 64, 48)]
            net.start("r2", ("rw", k), part, part, yp)

    def r_last(k):
        net.arrived(("rz", k), right.at[k, pl.ds(0, 384)], xn)
        net.arrived(("rw", k), right.at[k, pl.ds(0, 192)], yp)

    def weigh(k, c):
        p = jnp.dot(xp[c].reshape(512, 896), right[k], preferred_element_type=F32)
        w[512 * c : 512 * c + 512, :] = (zb[c] * p).astype(BF16)

    def mix(k, t):
        a = pl.ds(448 * t, 448)
        mp[k, a, :] = jnp.dot(xpt[a, :], w[...], preferred_element_type=F32)

    order = (2, 1, 3, 0)

    def e_start(k):
        for i, dx in enumerate(order):
            eys[k, i] = mp[k, rows(dx, 1, 48, 64), :].astype(BF16)
            net.start("ey", ("ey", k, dx), eys.at[k, i], eyr.at[k, i], yp)
            if dx:
                for o in range(2):
                    e1s[k, i, o] = mp[k, rows(dx, o, 0, 48), :].astype(BF16)
                net.start("e1", ("e1", k), e1s.at[k, i], e1r.at[k, i], at(dx, 0))

    def e_y(k, dx):
        i = order.index(dx)
        net.arrived(("ey", k, dx), eyr.at[k, i], yp)
        return mp[k, rows(dx, 0, 48, 64), :] + eyr[k, i].astype(F32)

    def e_two(k):
        for i, dx in enumerate(order[:3]):
            e2s[k, i] = e_y(k, dx).astype(BF16)
            net.start("e2", ("e2", k), e2s.at[k, i], e2r.at[k, i], at(dx, 0))

    def e_three(k):
        v = mp[k, rows(0, 1, 0, 48), :]
        net.arrived(("e1", k), e1r.at[k], xn)
        for i in range(3):
            v = v + e1r[k, i, 1].astype(F32)
        e3s[k] = v.astype(BF16)
        net.start("e3", ("e3", k), e3s.at[k], e3r.at[k], yp)

    def e_last(k):
        v = e_y(k, 0)
        net.arrived(("e2", k), e2r.at[k], xn)
        for i in range(3):
            v = v + e2r[k, i].astype(F32)
        u = mp[k, rows(0, 0, 0, 48), :]
        for i in range(3):
            u = u + e1r[k, i, 0].astype(F32)
        net.arrived(("e3", k), e3r.at[k], yp)
        return jnp.concatenate([u + e3r[k].astype(F32), v], axis=0)

    def ladder(k, v):
        gap = jnp.zeros((8, 512), F32)
        v = jnp.concatenate([v[:56], gap, v[56:], gap], axis=0).astype(BF16)
        for column in (1 - yl, yl):
            part = pl.ds(pl.multiple_of(column * 448, 64), 448)
            lad[k, part] = lax.dot_general(
                xqt[part, :], v, (((1,), (1,)), ((), ())), preferred_element_type=F32
            )
            if column is not yl:
                for dz in far + (0,):
                    j = gi(dz, 1)
                    u = lad[k, pl.ds(pl.multiple_of(j * 56, 8), 56), :]
                    fs[k, j] = u.astype(BF16)
                    net.start("fy", ("fy", k, dz), fs.at[k, j], fy.at[k, dz], yn)

    def fold(k):
        for dz in far + (0,):
            j = gi(dz, 0)
            net.arrived(("fy", k, dz), fy.at[k, dz], yn)
            v = lad[k, pl.ds(pl.multiple_of(j * 56, 8), 56), :] + fy[k, dz].astype(F32)
            if dz:
                fs[k, j] = v.astype(BF16)
                net.start("f", ("f", k), fs.at[k, j], fr.at[k, dz], up(dz))
            else:
                fins[k] = v

    def scoped(name, f, *args):
        with jax.named_scope(name):
            return f(*args)

    scoped("t00", t_forward, 0, 0)
    scoped("xp_y", xp_y)
    scoped("t01", t_forward, 0, 1)
    scoped("t07", t_forward, 0, 7)
    scoped("xq_y", xq_forward, 0, 1)
    with jax.named_scope("t0_xq"):
        for i, dz in enumerate((4, 3, 5, 2, 6)):
            t_forward(0, dz)
            if i < 3:
                xq_forward(*around[::-1][i])
    t_send(1)
    scoped("xp_step10", xp_step, 1, 0)
    scoped("xp_step11", xp_step, 1, 1)
    with jax.named_scope("first0a"):
        net.arrived(("xqm", 0), xq.at[yh, :, 1 - core], mate)
        t0 = gathered(0)
        r_send(0, first(0, t0, yh))
    with jax.named_scope("xq_far"):
        for dx, dy in around[2::-1]:
            xq_forward(dx, dy)
        net.arrived(("xqm", 1), xq.at[1 - yh, :, 1 - core], mate)
    with jax.named_scope("first0"):
        r_send(0, first(0, t0, 1 - yh))
    scoped("xp_step20", xp_step, 2, 0)
    scoped("xp_step21", xp_step, 2, 1)
    with jax.named_scope("xqt"):
        xqt[...] = jnp.transpose(xq[...].reshape(512, 896))
    with jax.named_scope("energies"):
        vcopy.wait()
        pcopy.wait()

        def run(start):
            r, off = start // 128, start % 128
            lane = lax.broadcasted_iota(jnp.int32, (8, 128), 1)
            one = jnp.broadcast_to(ve[pl.ds(r, 1), :], (8, 128))
            two = jnp.broadcast_to(ve[pl.ds(jnp.minimum(r + 1, 6), 1), :], (8, 128))
            shift = (128 - off) % 128
            return jnp.where(lane < 128 - off, pltpu.roll(one, shift, 1), pltpu.roll(two, shift, 1))

        first_e = run(b * 56)[0:1, :64]
        second_e = jnp.transpose(jnp.broadcast_to(run(g * 56)[0:1], (128, 128)))[:56, :64]
        both = second_e + first_e
        for k in range(4):
            base[k] = (both - pe[k]) * own_amp[k]
    with jax.named_scope("t1"):
        for dz in (0, 1, 7, 4, 3, 5, 2, 6):
            t_forward(1, dz)
    with jax.named_scope("z_order"):
        zcopy.wait()

        def swap(i, carry):
            block = pl.ds(pl.multiple_of(64 * i, 64), 64)
            v = [zb[core, block, 128 * c : 128 * c + 128] for c in range(4)]
            u = [pltpu.roll(c, 64, 1) for c in v]
            low = lax.broadcasted_iota(jnp.int32, (64, 128), 1) < 64
            zb[core, block, 0:128] = jnp.where(low, v[0], u[1])
            zb[core, block, 128:256] = jnp.where(low, v[2], u[3])
            zb[core, block, 256:384] = jnp.where(low, u[0], v[1])
            zb[core, block, 384:512] = jnp.where(low, u[2], v[3])
            return carry

        lax.fori_loop(0, 8, swap, 0)
    net.start("z", "z", zb.at[core], zb.at[core], mate)
    scoped("r_x01", r_x, 0, 1)
    scoped("xp_step30", xp_step, 3, 0)
    scoped("r_x03", r_x, 0, 3)
    scoped("xp_step31", xp_step, 3, 1)
    scoped("r_y0", r_y, 0)
    scoped("r_x02", r_x, 0, 2)
    with jax.named_scope("first1"):
        t1 = gathered(1)
        for half in range(2):
            first(1, t1, half)
        r_send(1, pl.ds(0, 512))
    scoped("xp_step40", xp_step, 4, 0)
    scoped("xp_step41", xp_step, 4, 1)
    with jax.named_scope("z_wait"):
        net.arrived("z", zb.at[1 - core], mate)
    with jax.named_scope("xpm_wait"):
        net.arrived("xpm", xp.at[1 - core], mate)
    with jax.named_scope("xpt"):
        for t in range(4):
            xpt[:, 256 * t : 256 * t + 256] = jnp.transpose(
                xp[t // 2, pl.ds(8 * (t % 2), 8)].reshape(256, 896)
            )
    scoped("r_last0", r_last, 0)
    scoped("weigh00", weigh, 0, 0)
    scoped("r_x11", r_x, 1, 1)
    scoped("r_x13", r_x, 1, 3)
    scoped("r_y1", r_y, 1)
    scoped("weigh01", weigh, 0, 1)
    scoped("r_x12", r_x, 1, 2)
    scoped("mix00", mix, 0, 0)
    scoped("mix01", mix, 0, 1)
    scoped("e_start0", e_start, 0)
    scoped("r_last1", r_last, 1)
    scoped("weigh10", weigh, 1, 0)
    scoped("weigh11", weigh, 1, 1)
    scoped("mix10", mix, 1, 0)
    scoped("mix11", mix, 1, 1)
    scoped("e_start1", e_start, 1)
    scoped("e_two0", e_two, 0)
    scoped("e_three0", e_three, 0)
    scoped("e_two1", e_two, 1)
    scoped("e_three1", e_three, 1)
    v0 = scoped("e_last0", e_last, 0)
    scoped("ladder0", ladder, 0, v0)
    v1 = scoped("e_last1", e_last, 1)
    scoped("ladder1", ladder, 1, v1)
    scoped("fold0", fold, 0)
    scoped("fold1", fold, 1)
    for k in range(2):
        total = fins[k]
        with jax.named_scope(f"f_wait{k}"):
            net.arrived(("f", k), fr.at[k, pl.ds(1, 7)], zn)
            for dz in far:
                total = total + fr[k, dz].astype(F32)
        fins[k] = total
        net.start("fin", ("fin", k), fins.at[k], finr.at[k], mate)
    def finish(pair, v):
        v = jnp.where(core == 0, v[:, :64], v[:, 64:]) + base[pair]
        out_ref[pair] = v[:, :56]

    for k in range(2):
        finish(2 * core + k, fins[k])
    with jax.named_scope("fin"):
        for k in range(2):
            net.arrived(("fin", k), finr.at[k], mate)
            finish(2 * (1 - core) + k, finr[k])
    with jax.named_scope("close"):
        for kind, whole in (
            ("t", tall.at[:, 0, pl.ds(0, 15)]), ("ty", tall.at[:, 0]), ("x", xq),
            ("xp", xp.at[0, pl.ds(0, 14)]), ("xpm", xp.at[0]), ("z", zb.at[0]),
            ("r", right.at[0]), ("r2", right.at[0, pl.ds(0, 672)]), ("ey", eys), ("e1", e1s),
            ("e2", e2s), ("e3", e3s), ("fy", fy), ("f", fr.at[:, pl.ds(0, 7)]), ("fin", fins),
        ):
            net.sent(kind, whole, mate)


def local(amplitudes, grid_factor, metric, virt_energy, pair_energy):
    rows, pairs, cols = amplitudes.shape
    hbm = pl.BlockSpec(memory_space=pltpu.HBM)
    out = pl.pallas_call(
        kernel,
        out_shape=pltpu.VMEM((pairs, cols, rows), F32),
        in_specs=[hbm] * 5,
        out_specs=pl.BlockSpec(memory_space=pltpu.VMEM),
        scratch_shapes=[
            pltpu.VMEM((56, 4, 56), BF16),
            pltpu.VMEM((32, 896), BF16),
            pltpu.VMEM((8, 128), F32),
            pltpu.SMEM((4,), F32),
            pltpu.VMEM((4, 32, 128), BF16),
            pltpu.VMEM((4, 56, 64), F32),
            pltpu.VMEM((4, 56, 64), F32),
            pltpu.VMEM((2, 2, 16, 32, 128), BF16),
            pltpu.VMEM((2, 4, 2, 32, 896), BF16),
            pltpu.VMEM((896, 512), BF16),
            pltpu.VMEM((2, 16, 32, 896), BF16),
            pltpu.VMEM((896, 1024), BF16),
            pltpu.VMEM((2, 512, 512), F32),
            pltpu.VMEM((2, 896, 512), BF16),
            pltpu.VMEM((1024, 512), BF16),
            pltpu.VMEM((2, 896, 512), F32),
            pltpu.VMEM((2, 3, 2, 48, 512), BF16),
            pltpu.VMEM((2, 3, 2, 48, 512), BF16),
            pltpu.VMEM((2, 3, 64, 512), BF16),
            pltpu.VMEM((2, 3, 64, 512), BF16),
            pltpu.VMEM((2, 48, 512), BF16),
            pltpu.VMEM((2, 48, 512), BF16),
            pltpu.VMEM((2, 4, 64, 512), BF16),
            pltpu.VMEM((2, 4, 64, 512), BF16),
            pltpu.VMEM((2, 896, 128), F32),
            pltpu.VMEM((2, 16, 56, 128), BF16),
            pltpu.VMEM((2, 8, 56, 128), BF16),
            pltpu.VMEM((2, 8, 56, 128), BF16),
            pltpu.VMEM((2, 56, 128), F32),
            pltpu.VMEM((2, 56, 128), F32),
            pltpu.SemaphoreType.DMA((KINDS,)),
            pltpu.SemaphoreType.DMA((NAMES,)),
            pltpu.SemaphoreType.DMA((5,)),
        ],
        compiler_params=pltpu.CompilerParams(
            collective_id=0, has_side_effects=True, vmem_limit_bytes=65000 * 1024
        ),
    )(amplitudes, grid_factor, metric, virt_energy.reshape(7, 128), pair_energy)
    return jnp.transpose(out, (2, 0, 1))


def solution(mesh):
    in_specs = (P("blk", None, "grp"), P(("blk", "grp"), None), P("blk", "grp", None), P(), P())
    return jax.shard_map(
        local, mesh=mesh, in_specs=in_specs, out_specs=P("blk", None, "grp"), check_vma=False
    )
```
